8 devices in a mesh: replica: 4 (over z, y, x), fsdp: 2 (over core).
Axes of the slice: x: 2, y: 2, z: 1, core: 2. Of those that a mesh axis runs over, the one named last changes fastest.
Arguments:
- block_in: bfloat16 [1, 32768, 2048], P(None, ('replica', 'fsdp'))
- grad_out: bfloat16 [32768, 2048], P(('replica', 'fsdp'))
- w_up: bfloat16 [1, 2048, 8192], P(None, 'fsdp')
- w_lin: bfloat16 [1, 2048, 8192], P(None, 'fsdp')
- w_down: bfloat16 [1, 8192, 2048], P(None, 'fsdp')
Outputs:
- output 1: float32 [1, 2048, 8192], P(None, 'fsdp')
- output 2: float32 [1, 2048, 8192], P(None, 'fsdp')
- output 3: float32 [1, 8192, 2048], P(None, 'fsdp')
- output 4: bfloat16 [32768, 2048], P(('replica', 'fsdp'))
All inputs are finite; a program needn't handle non-finite values.
Results may differ from the reference program's by a relative error of at most 0.001.
Values are sent between devices in bfloat16 or wider.
A program may use at most 1 GiB of HBM per device.

```python
import jax
import jax.numpy as jnp
from jax import lax

D = 2048
FF = 8192
LAYERS = 1
TOK_DEV = 4096
REPLICA = 4
FSDP = 2
TOKENS = TOK_DEV * REPLICA * FSDP
NUM_BLOCKS = REPLICA * FSDP
NORM_EPS = 1e-5


def setup_inputs(seed: int = 0) -> dict:
    key_list = jax.random.split(jax.random.key(seed), 5)
    block_in = jax.random.normal(key_list[0], (LAYERS, TOKENS, D), jnp.float32).astype(jnp.bfloat16)
    grad_out = jax.random.normal(key_list[1], (TOKENS, D), jnp.float32).astype(jnp.bfloat16)
    w_up = (jax.random.normal(key_list[2], (LAYERS, D, FF), jnp.float32) * D ** -0.5).astype(jnp.bfloat16)
    w_lin = (jax.random.normal(key_list[3], (LAYERS, D, FF), jnp.float32) * D ** -0.5).astype(jnp.bfloat16)
    w_down = (jax.random.normal(key_list[4], (LAYERS, FF, D), jnp.float32) * (0.5 * FF ** -0.5)).astype(jnp.bfloat16)
    return {'block_in': block_in, 'grad_out': grad_out, 'w_up': w_up, 'w_lin': w_lin, 'w_down': w_down}


def layer_grad(h_in, grad_acc, up_w, lin_w, down_w):
    h_f32 = h_in.astype(jnp.float32)
    inv_rms = lax.rsqrt(jnp.mean(h_f32 * h_f32, axis=-1, keepdims=True) + NORM_EPS)
    normed = h_f32 * inv_rms
    normed_b = normed.astype(jnp.bfloat16)
    pre_up = jnp.dot(normed_b, up_w, preferred_element_type=jnp.float32)
    pre_lin = jnp.dot(normed_b, lin_w, preferred_element_type=jnp.float32)
    up_sig = jax.nn.sigmoid(pre_up)
    up_act = pre_up * up_sig
    act_b = (up_act * pre_lin).astype(jnp.bfloat16)
    grad_b = grad_acc.astype(jnp.bfloat16)
    d_act = jnp.dot(grad_b, down_w.T, preferred_element_type=jnp.float32)
    d_up = (d_act * pre_lin * up_sig * (1.0 + pre_up * (1.0 - up_sig))).astype(jnp.bfloat16)
    d_lin = (d_act * up_act).astype(jnp.bfloat16)
    g_down = jnp.dot(act_b.T, grad_b, preferred_element_type=jnp.float32)
    g_up = jnp.dot(normed_b.T, d_up, preferred_element_type=jnp.float32)
    g_lin = jnp.dot(normed_b.T, d_lin, preferred_element_type=jnp.float32)
    d_norm = jnp.dot(d_up, up_w.T, preferred_element_type=jnp.float32) + jnp.dot(d_lin, lin_w.T, preferred_element_type=jnp.float32)
    d_h = inv_rms * (d_norm - normed * jnp.mean(d_norm * normed, axis=-1, keepdims=True))
    return grad_acc + d_h, g_up, g_lin, g_down


def reference(block_in, grad_out, w_up, w_lin, w_down):
    blocks_in = block_in.reshape(LAYERS, NUM_BLOCKS, TOK_DEV, D).transpose(1, 0, 2, 3)
    blocks_grad = grad_out.reshape(NUM_BLOCKS, TOK_DEV, D)

    def block_step(grad_sums, block_xs):
        h_block, g_block = block_xs

        def layer_step(grad_acc, layer_xs):
            h_layer, up_w, lin_w, down_w = layer_xs
            new_grad, g_up, g_lin, g_down = layer_grad(h_layer, grad_acc, up_w, lin_w, down_w)
            return new_grad, (g_up, g_lin, g_down)

        final_grad, layer_grads = lax.scan(layer_step, g_block.astype(jnp.float32), (h_block, w_up, w_lin, w_down), reverse=True)
        new_sums = tuple(old_part + new_part for old_part, new_part in zip(grad_sums, layer_grads))
        return new_sums, final_grad.astype(jnp.bfloat16)

    zero_sums = (jnp.zeros((LAYERS, D, FF), jnp.float32), jnp.zeros((LAYERS, D, FF), jnp.float32), jnp.zeros((LAYERS, FF, D), jnp.float32))
    grad_sums, grad_blocks = lax.scan(block_step, zero_sums, (blocks_in, blocks_grad))
    return grad_sums[0], grad_sums[1], grad_sums[2], grad_blocks.reshape(TOKENS, D)
```

```python
import functools

import jax
import jax.numpy as jnp
from jax import lax
from jax.experimental import pallas as pl
from jax.experimental.pallas import tpu as pltpu
from jax.sharding import PartitionSpec as P

NORM_EPS = 1e-5
BF16 = jnp.bfloat16
F32 = jnp.float32
VMEM_LIMIT = 62 * 1024 * 1024
UNIT = 32
SLOTS = 4
F_SLOTS = 8
G_SLOTS = 16
CHUNKS = ((256, 256, 0), (3840, 256, 72))
EARLY = 768
TILE = 512
ANY = pl.BlockSpec(memory_space=pl.ANY)
MESH = pl.DeviceIdType.MESH


def SMALL():
    global CHUNKS, EARLY
    CHUNKS = ((128, 128, 0), (896, 128, 8))
    EARLY = 384


def dot_nn(a, b):
    return lax.dot_general(a, b, (((1,), (0,)), ((), ())), preferred_element_type=F32)


def dot_nt(a, b):
    return lax.dot_general(a, b, (((1,), (1,)), ((), ())), preferred_element_type=F32)


def dot_tn(a, b):
    return lax.dot_general(a, b, (((0,), (0,)), ((), ())), preferred_element_type=F32)


def exchange(w1o, w3o, w2o, into, lo, hi, send_sem, recv_sem):
    r, k, _, _ = position()
    f_half = w1o.shape[1] // 2
    pairs = [(src.at[:, pl.ds(p * f_half + lo, hi - lo)], dst.at[:, pl.ds(p * f_half + lo, hi - lo)])
             for src, dst in ((w1o, into[0]), (w3o, into[1])) for p in range(2)]
    pairs.append((w2o.at[pl.ds(lo, hi - lo), :], into[2].at[pl.ds(lo, hi - lo), :]))
    return [pltpu.make_async_remote_copy(
        src_ref=src, dst_ref=dst, send_sem=send_sem.at[num], recv_sem=recv_sem.at[num],
        device_id=(r, 1 - k), device_id_type=MESH) for num, (src, dst) in enumerate(pairs)]


def norm_kernel(n_tiles, h_ref, w1o, w3o, w2o, n_ref, w1r, w3r, w2r, send_sem, recv_sem):
    i = pl.program_id(0)
    r, k, _, _ = position()
    args = (w1o, w3o, w2o, (w1r, w3r, w2r), 0, EARLY, send_sem, recv_sem)

    @pl.when(i == 0)
    def _():
        barrier = pltpu.get_barrier_semaphore()
        pl.semaphore_signal(barrier, inc=1, device_id=(r, 1 - k), device_id_type=MESH)
        pl.semaphore_wait(barrier, 1)
        for copy in exchange(*args):
            copy.start()

    half = h_ref.shape[1] // 2
    h = h_ref[...].astype(F32)
    inv_rms = lax.rsqrt(jnp.mean(h * h, axis=-1, keepdims=True) + NORM_EPS)
    y = (h * inv_rms).astype(BF16)
    first = k == 0
    n_ref[:, :half] = jnp.where(first, y[:, :half], y[:, half:])
    n_ref[:, half:] = jnp.where(first, y[:, half:], y[:, :half])

    @pl.when(i == n_tiles - 1)
    def _():
        for copy in exchange(*args):
            copy.wait()


def norm_call(h, own):
    tokens, dim = h.shape
    tile = 512
    spec = pl.BlockSpec((tile, dim), lambda i: (i, 0))
    return pl.pallas_call(
        functools.partial(norm_kernel, tokens // tile),
        grid=(tokens // tile,),
        in_specs=[spec] + [ANY] * 3,
        out_specs=[spec] + [ANY] * 3,
        scratch_shapes=[pltpu.SemaphoreType.DMA((5,)), pltpu.SemaphoreType.DMA((5,))],
        out_shape=[jax.ShapeDtypeStruct((tokens, dim), BF16)] + [jax.ShapeDtypeStruct(w.shape, BF16) for w in own],
        compiler_params=pltpu.CompilerParams(vmem_limit_bytes=VMEM_LIMIT, collective_id=8, has_side_effects=True),
        cost_estimate=pl.CostEstimate(flops=6 * tokens * dim, bytes_accessed=4 * tokens * dim, transcendentals=tokens),
        name='norm',
    )(h, *own)


def rs_scratch(dim):
    rows = 3 * UNIT
    return [
        pltpu.VMEM((SLOTS, rows, dim), F32),
        pltpu.VMEM((SLOTS, rows, dim), F32),
        pltpu.VMEM((SLOTS, rows, dim // 2), F32),
        pltpu.VMEM((SLOTS, rows, dim // 2), F32),
        pltpu.VMEM((SLOTS, rows, dim // 4), F32),
        pltpu.VMEM((F_SLOTS, rows, dim // 4), F32),
        pltpu.SemaphoreType.DMA((SLOTS, 6)),
        pltpu.SemaphoreType.DMA((SLOTS, 4)),
        pltpu.SemaphoreType.DMA((SLOTS, 4)),
        pltpu.SemaphoreType.DMA((F_SLOTS,)),
        pltpu.SemaphoreType.DMA((G_SLOTS, 6)),
        pltpu.SemaphoreType.DMA((G_SLOTS, 6)),
        pltpu.SemaphoreType.REGULAR((4,)),
    ]


def position():
    r = lax.axis_index('replica')
    k = lax.axis_index('fsdp')
    x, y = lax.rem(r, 2), lax.div(r, 2)
    return r, k, x, y


def enter(step):
    r, k, x, y = position()

    @pl.when(step == 0)
    def _():
        barrier = pltpu.get_barrier_semaphore()
        for peer in ((r, 1 - k), (r + 1 - 2 * x, k), (r + 2 - 4 * y, k)):
            pl.semaphore_signal(barrier, inc=1, device_id=peer, device_id_type=MESH)
        pl.semaphore_wait(barrier, 3)


def ticks(step, n_grid, n_units, first, gather, z_own, z_in, f_out, scratch):
    own_buf, in_buf, r1, y2, r2, f_buf, load_sem, send_sem, recv_sem, out_sem, g_send, g_recv, credit = scratch
    r, k, x, y = position()
    at_x, at_y = (r + 1 - 2 * x, k), (r + 2 - 4 * y, k)
    dim = own_buf.shape[2]
    quarter, eighth = dim // 4, dim // 8
    n_ticks = n_units + (11 if gather else 7)

    def loads(u):
        slot = lax.rem(u, SLOTS)
        row = pl.multiple_of((first + u) * UNIT, UNIT)
        copies = []
        for part in range(3):
            dst = pl.ds(part * UNIT, UNIT)
            copies.append(pltpu.make_async_copy(z_own.at[part, pl.ds(row, UNIT), :], own_buf.at[slot, dst, :], load_sem.at[slot, part]))
            copies.append(pltpu.make_async_copy(z_in.at[part, pl.ds(row, UNIT), :], in_buf.at[slot, dst, :], load_sem.at[slot, 3 + part]))
        return copies

    def lanes(base, index, width):
        return pl.ds(pl.multiple_of(base + index * width, 128), width)

    def first_hop(u):
        slot = lax.rem(u, SLOTS)
        out = []
        for i, (base, index, peer, col) in enumerate(((0, 1 - x, at_x, 0), (dim // 2, 1 - y, at_y, quarter))):
            out.append(pltpu.make_async_remote_copy(
                src_ref=own_buf.at[slot, :, lanes(base, index, quarter)], dst_ref=r1.at[slot, :, pl.ds(col, quarter)],
                send_sem=send_sem.at[slot, i], recv_sem=recv_sem.at[slot, i], device_id=peer, device_id_type=MESH))
        return out

    def second_hop(u):
        slot = lax.rem(u, SLOTS)
        out = []
        for i, (base, index, peer, col) in enumerate(((0, 1 - y, at_y, 0), (quarter, 1 - x, at_x, eighth))):
            out.append(pltpu.make_async_remote_copy(
                src_ref=y2.at[slot, :, lanes(base, index, eighth)], dst_ref=r2.at[slot, :, pl.ds(col, eighth)],
                send_sem=send_sem.at[slot, 2 + i], recv_sem=recv_sem.at[slot, 2 + i], device_id=peer, device_id_type=MESH))
        return out

    def stores(u):
        slot = lax.rem(u, F_SLOTS)
        dst = f_out.at[r, u] if gather else f_out.at[u]
        return pltpu.make_async_copy(f_buf.at[slot], dst, out_sem.at[slot])

    def spread(u, num, src, origin, col, peer):
        slot = lax.rem(u, G_SLOTS)
        return pltpu.make_async_remote_copy(
            src_ref=src, dst_ref=f_out.at[origin, u, :, pl.ds(col, eighth)], send_sem=g_send.at[slot, num],
            recv_sem=g_recv.at[slot, num], device_id=peer, device_id_type=MESH)

    def third_hop(u):
        slot = lax.rem(u, F_SLOTS)
        return [spread(u, i, f_buf.at[slot, :, pl.ds(col, eighth)], r, col, peer)
                for i, (col, peer) in enumerate(((0, at_y), (eighth, at_x)))]

    def fourth_hop(u):
        slot = lax.rem(u, F_SLOTS)
        return [spread(u, 2 + i, f_buf.at[slot, :, pl.ds(col, eighth)], r, col, peer)
                for i, (col, peer) in enumerate(((0, at_x), (eighth, at_y)))]

    def forward(u):
        return [spread(u, 4 + i, f_out.at[origin, u, :, pl.ds(col, eighth)], origin, col, peer)
                for i, (origin, col, peer) in enumerate(((at_y[0], 0, at_x), (at_x[0], eighth, at_y)))]

    def stage(tick, lag, fn):
        u = tick - lag

        @pl.when(jnp.logical_and(u >= 0, u < n_units))
        def _():
            fn(u, lax.rem(u, SLOTS))

    def do_load(u, slot):
        for copy in loads(u):
            copy.start()

    def do_first(u, slot):
        for copy in loads(u):
            copy.wait()
        own_buf[slot] = own_buf[slot] + in_buf[slot]

        @pl.when(u >= SLOTS)
        def _():
            pl.semaphore_wait(credit.at[0], 1)
            pl.semaphore_wait(credit.at[1], 1)

        for copy in first_hop(u):
            copy.start()

    def do_second(u, slot):
        for copy in first_hop(u):
            copy.wait()
        y2[slot, :, :quarter] = own_buf[slot, :, lanes(0, x, quarter)] + r1[slot, :, :quarter]
        y2[slot, :, quarter:] = own_buf[slot, :, lanes(dim // 2, y, quarter)] + r1[slot, :, quarter:]

        @pl.when(u < n_units - SLOTS)
        def _():
            pl.semaphore_signal(credit.at[0], inc=1, device_id=at_x, device_id_type=MESH)
            pl.semaphore_signal(credit.at[1], inc=1, device_id=at_y, device_id_type=MESH)

        @pl.when(u >= SLOTS)
        def _():
            pl.semaphore_wait(credit.at[2], 1)
            pl.semaphore_wait(credit.at[3], 1)

        for copy in second_hop(u):
            copy.start()

    def do_third(u, slot):
        for copy in second_hop(u):
            copy.wait()
        f_slot = lax.rem(u, F_SLOTS)
        f_buf[f_slot, :, :eighth] = y2[slot, :, lanes(0, y, eighth)] + r2[slot, :, :eighth]
        f_buf[f_slot, :, eighth:] = y2[slot, :, lanes(quarter, x, eighth)] + r2[slot, :, eighth:]

        @pl.when(u < n_units - SLOTS)
        def _():
            pl.semaphore_signal(credit.at[2], inc=1, device_id=at_y, device_id_type=MESH)
            pl.semaphore_signal(credit.at[3], inc=1, device_id=at_x, device_id_type=MESH)

        stores(u).start()
        if gather:
            for copy in third_hop(u) + fourth_hop(u):
                copy.start()

    def do_forward(u, slot):
        for copy in third_hop(u):
            copy.wait()
        for copy in forward(u):
            copy.start()

    def do_end(u, slot):
        stores(u).wait()
        if gather:
            for copy in fourth_hop(u) + forward(u):
                copy.wait()

    def tick(t, carry):
        if gather:
            stage(t, 10, do_end)
            stage(t, 7, do_forward)
        else:
            stage(t, 6, do_end)
        stage(t, 5, do_third)
        stage(t, 3, do_second)
        stage(t, 1, do_first)
        stage(t, 0, do_load)
        return carry

    lax.fori_loop((step * n_ticks) // n_grid, ((step + 1) * n_ticks) // n_grid, tick, 0)


def chunk_kernel(sh, n_steps, n_tiles, n_alias, start, n_units, unit_off, n_ref, g_ref, w1o, w3o, w2o, *rest):
    last = n_alias > 0
    if not last:
        w1r, w3r, w2r = rest[:3]
        rest = rest[3:]
    rest = rest[n_alias:]
    du_0, du_1, dv_0, dv_1, z_own, z_in = rest[:6]
    n_out = 6
    if last:
        into = w1r, w3r, w2r = rest[6:9]
        f_out = rest[9]
        n_out = 10
    w13, w2c, acc13, acc2, w_sem, out_sem, d_send, d_recv, p_send, p_recv = rest[n_out:n_out + 10]
    scratch = rest[n_out + 10:]
    half = w1o.shape[0]
    f_half = w1o.shape[1] // 2
    wide = 2 * sh
    j = pl.program_id(0)
    i = pl.program_id(1)
    slot = lax.rem(j, 2)
    r, k, _, _ = position()
    own_row = pl.multiple_of(k * sh, 128)
    oth_row = pl.multiple_of((1 - k) * sh, 128)
    enter(j * n_tiles + i)
    if n_units:
        ticks(j * n_tiles + i, n_steps * n_tiles, n_units, unit_off, True, z_own, z_in, f_out, scratch)

    def fetches(step, buf):
        copies = []

        def add(src, dst):
            copies.append(pltpu.make_async_copy(src, dst, w_sem.at[buf, len(copies)]))

        at = pl.multiple_of(start + step * sh, 128)
        for own_src, oth_src, col in ((w1o, w1r, 0), (w3o, w3r, wide)):
            for src, row in ((own_src, 0), (oth_src, half)):
                for p in range(2):
                    add(src.at[:, pl.ds(p * f_half + at, sh)], w13.at[buf, pl.ds(row, half), pl.ds(col + p * sh, sh)])
        for src, row in ((w2o, own_row), (w2r, oth_row)):
            add(src.at[pl.ds(at, sh), :], w2c.at[buf, pl.ds(row, sh), :])
        return copies

    def drains(step):
        row = pl.multiple_of(start + step * sh, 128)
        local, remote = [], []

        def add(keep, send, part, lanes):
            num = len(local)
            local.append(pltpu.make_async_copy(keep, z_own.at[part, pl.ds(row, sh), lanes], out_sem.at[num]))
            remote.append(pltpu.make_async_remote_copy(
                src_ref=send, dst_ref=z_in.at[part, pl.ds(row, sh), lanes], send_sem=d_send.at[num], recv_sem=d_recv.at[step, num],
                device_id=(r, 1 - k), device_id_type=MESH))

        for part in range(2):
            for p in range(2):
                src = pl.ds(part * wide + p * sh, sh)
                add(acc13.at[src, pl.ds(0, half)], acc13.at[src, pl.ds(half, half)], part, pl.ds(p * half, half))
        add(acc2.at[pl.ds(own_row, sh), :], acc2.at[pl.ds(oth_row, sh), :], 2, pl.ds(0, 2 * half))
        return local, remote

    def finish(step):
        local, remote = drains(step)
        for copy in local:
            copy.wait()
        for copy in remote:
            copy.wait()

    if last:
        args = (w1o, w3o, w2o, into, EARLY, f_half, p_send, p_recv)

        @pl.when(jnp.logical_and(i == 0, j == 0))
        def _():
            for copy in exchange(*args):
                copy.start()

        @pl.when(jnp.logical_and(i == 0, j == 1))
        def _():
            for copy in exchange(*args):
                copy.wait()

    @pl.when(i == 0)
    def _():
        @pl.when(j == 0)
        def _():
            for copy in fetches(0, 0):
                copy.start()

        for copy in fetches(j, slot):
            copy.wait()

        @pl.when(j + 1 < n_steps)
        def _():
            for copy in fetches(j + 1, 1 - slot):
                copy.start()

    n = n_ref[...]
    g = g_ref[...]
    uv = dot_nn(n, w13[slot])
    da = dot_nt(g, w2c[slot])
    u = uv[:, :wide]
    v = uv[:, wide:]
    sig = jax.nn.sigmoid(u)
    up_act = u * sig
    act = (up_act * v).astype(BF16)
    du = (da * v * sig * (1.0 + u * (1.0 - sig))).astype(BF16)
    dv = (da * up_act).astype(BF16)
    du_0[...] = du[:, :sh]
    du_1[...] = du[:, sh:]
    dv_0[...] = dv[:, :sh]
    dv_1[...] = dv[:, sh:]

    @pl.when(jnp.logical_and(i == 0, j > 0))
    def _():
        finish(j - 1)

    @pl.when(i == 0)
    def _():
        acc13[...] = jnp.zeros_like(acc13)
        acc2[...] = jnp.zeros_like(acc2)

    acc2[...] += dot_tn(act, g)
    acc13[...] += dot_tn(jnp.concatenate([du, dv], axis=1), n)

    @pl.when(i == n_tiles - 1)
    def _():
        local, remote = drains(j)
        for copy in remote + local:
            copy.start()

        @pl.when(j == n_steps - 1)
        def _():
            finish(j)


def chunk_call(c, n, g, own, recv, bufs, start, units, unit_off):
    tokens, dim = n.shape
    f_half = own[0].shape[1] // 2
    cols, sh, _ = CHUNKS[c]
    tile = TILE
    n_steps, n_tiles = cols // sh, tokens // tile
    off = start // sh
    tile_spec = pl.BlockSpec((tile, sh), lambda j, i: (i, off + j))
    row_spec = pl.BlockSpec((tile, dim), lambda j, i: (i, 0))
    big = jax.ShapeDtypeStruct((tokens, f_half), BF16)
    z = jax.ShapeDtypeStruct((3, f_half, dim), F32)
    shapes = [big] * 4 + [z] * 2
    if bufs:
        shapes += [jax.ShapeDtypeStruct(w.shape, BF16) for w in own]
        shapes.append(jax.ShapeDtypeStruct((4, units, 3 * UNIT, dim // 4), F32))
        bufs, recv = bufs + recv, ()
    n_alias = len(bufs)
    return pl.pallas_call(
        functools.partial(chunk_kernel, sh, n_steps, n_tiles, n_alias, start, units, unit_off),
        grid=(n_steps, n_tiles),
        in_specs=[row_spec, row_spec] + [ANY] * (3 + len(recv) + n_alias),
        out_specs=[tile_spec] * 4 + [ANY] * (len(shapes) - 4),
        scratch_shapes=[
            pltpu.VMEM((2, dim, 4 * sh), BF16),
            pltpu.VMEM((2, 2 * sh, dim), BF16),
            pltpu.VMEM((4 * sh, dim), F32),
            pltpu.VMEM((2 * sh, dim), F32),
            pltpu.SemaphoreType.DMA((2, 10)),
            pltpu.SemaphoreType.DMA((5,)),
            pltpu.SemaphoreType.DMA((5,)),
            pltpu.SemaphoreType.DMA((n_steps, 5)),
            pltpu.SemaphoreType.DMA((5,)),
            pltpu.SemaphoreType.DMA((5,)),
        ] + (rs_scratch(dim) if units else []),
        out_shape=shapes,
        input_output_aliases={5 + len(recv) + a: a for a in range(n_alias)},
        compiler_params=pltpu.CompilerParams(
            vmem_limit_bytes=VMEM_LIMIT, dimension_semantics=('arbitrary', 'arbitrary'), collective_id=c, has_side_effects=True),
        cost_estimate=pl.CostEstimate(flops=24 * tokens * dim * cols, bytes_accessed=n_steps * 4 * tokens * dim + 24 * dim * cols, transcendentals=tokens * 2 * cols),
        name=f'chunk{c}',
    )(n, g, *own, *recv, *bufs)


def place_kernel(n_any, z, *rest):
    out1, out3, out2 = rest[n_any:]
    p = pl.program_id(1)
    _, n_units, _, eighth = z.shape
    rows = n_units * UNIT
    for r in range(4):
        x, y = r % 2, r // 2
        for half, index in ((0, 2 * x + y), (1, 2 * y + x)):
            @pl.when(p == half)
            def _():
                at = pl.ds(index * eighth, eighth)
                out1[at, :] = z[r, :, :UNIT, :].reshape(rows, eighth).T
                out3[at, :] = z[r, :, UNIT:2 * UNIT, :].reshape(rows, eighth).T
                out2[:, at] = z[r, :, 2 * UNIT:, :].reshape(rows, eighth)


def place_call(z, outs, after, half, f_half, first_unit, name):
    dim = 2 * half
    units = z.shape[1]
    group = 8 if units % 8 == 0 and first_unit % 8 == 0 else 4
    sb = group * UNIT
    first, f_blocks = first_unit // group, f_half // sb
    n_alias = len(outs)
    side = jax.ShapeDtypeStruct((half, 2 * f_half), F32)
    side_spec = pl.BlockSpec((half, sb), lambda j, p: (0, p * f_blocks + first + j))
    return pl.pallas_call(
        functools.partial(place_kernel, n_alias + len(after)),
        grid=(units // group, 2),
        in_specs=[pl.BlockSpec((4, group, 3 * UNIT, dim // 8), lambda j, p: (0, j, 0, p))] + [ANY] * (n_alias + len(after)),
        out_specs=[side_spec, side_spec, pl.BlockSpec((sb, half), lambda j, p: (first + j, p))],
        out_shape=[side, side, jax.ShapeDtypeStruct((f_half, dim), F32)],
        input_output_aliases={1 + a: a for a in range(n_alias)},
        compiler_params=pltpu.CompilerParams(vmem_limit_bytes=VMEM_LIMIT, dimension_semantics=('arbitrary', 'arbitrary')),
        cost_estimate=pl.CostEstimate(flops=3 * units * UNIT * dim, bytes_accessed=24 * units * UNIT * dim, transcendentals=0),
        name=name,
    )(z, *outs, *after)


def dn_kernel(n_tiles, n_steps, n_alias, n_units, unit_off, *refs):
    (du_0, du_1, dv_0, dv_1, w1o_0, w1o_1, w1r_0, w1r_1, w3o_0, w3o_1, w3r_0, w3r_1, h_ref, g_ref, z_own, z_in) = refs[:16]
    rest = refs[16 + n_alias:]
    out_ref = rest[0]
    n_out = 2 if n_units else 1
    acc_own, acc_oth = rest[n_out:n_out + 2]
    f = pl.program_id(1)
    half = acc_own.shape[1]
    if n_units:
        step = pl.program_id(0) * n_steps + f
        enter(step)
        ticks(step, n_tiles * n_steps, n_units, unit_off, False, z_own, z_in, rest[1], rest[n_out + 2:])

    @pl.when(f == 0)
    def _():
        acc_own[...] = jnp.zeros_like(acc_own)
        acc_oth[...] = jnp.zeros_like(acc_oth)

    acc_own[...] += (dot_nt(du_0[...], w1o_0[...]) + dot_nt(du_1[...], w1o_1[...])
                     + dot_nt(dv_0[...], w3o_0[...]) + dot_nt(dv_1[...], w3o_1[...]))
    acc_oth[...] += (dot_nt(du_0[...], w1r_0[...]) + dot_nt(du_1[...], w1r_1[...])
                     + dot_nt(dv_0[...], w3r_0[...]) + dot_nt(dv_1[...], w3r_1[...]))

    @pl.when(f == n_steps - 1)
    def _():
        rows = 256
        first = lax.axis_index('fsdp') == 0
        for t in range(out_ref.shape[0] // rows):
            sl = pl.ds(t * rows, rows)
            h = h_ref[sl, :].astype(F32)
            inv_rms = lax.rsqrt(jnp.mean(h * h, axis=-1, keepdims=True) + NORM_EPS)
            y = h * inv_rms
            own, oth = acc_own[sl, :], acc_oth[sl, :]
            d = jnp.concatenate([jnp.where(first, own, oth), jnp.where(first, oth, own)], axis=1)
            mean = jnp.mean(d * y, axis=-1, keepdims=True)
            out_ref[sl, :] = (g_ref[sl, :].astype(F32) + inv_rms * (d - y * mean)).astype(BF16)


def dn_call(c, dus, w1o, w1r, w3o, w3r, h, g, z, bufs, tile_off, n_tiles, units, unit_off):
    tokens, dim = h.shape
    half = dim // 2
    tile, fb = 512, 512
    n_steps = dus[0].shape[1] // fb
    d_spec = pl.BlockSpec((tile, fb), lambda i, f: (tile_off + i, f))
    w_0 = pl.BlockSpec((half, fb), lambda i, f: (0, f))
    w_1 = pl.BlockSpec((half, fb), lambda i, f: (0, n_steps + f))
    row_spec = pl.BlockSpec((tile, dim), lambda i, f: (tile_off + i, 0))
    n_alias = len(bufs)
    f_out = [jax.ShapeDtypeStruct((units, 3 * UNIT, dim // 4), F32)] if units else []
    extra = dict(collective_id=c, has_side_effects=True) if units else {}
    return pl.pallas_call(
        functools.partial(dn_kernel, n_tiles, n_steps, n_alias, units, unit_off),
        grid=(n_tiles, n_steps),
        in_specs=[d_spec] * 4 + [w_0, w_1] * 4 + [row_spec, row_spec] + [ANY] * (2 + n_alias),
        out_specs=[row_spec] + [ANY] * len(f_out),
        scratch_shapes=[pltpu.VMEM((tile, half), F32), pltpu.VMEM((tile, half), F32)] + (rs_scratch(dim) if units else []),
        out_shape=[jax.ShapeDtypeStruct((tokens, dim), BF16)] + f_out,
        input_output_aliases={16 + a: a for a in range(n_alias)},
        compiler_params=pltpu.CompilerParams(vmem_limit_bytes=VMEM_LIMIT, dimension_semantics=('arbitrary', 'arbitrary'), **extra),
        cost_estimate=pl.CostEstimate(flops=8 * n_tiles * tile * dim * n_steps * fb, bytes_accessed=8 * n_tiles * tile * n_steps * fb + 8 * n_tiles * dim * n_steps * fb, transcendentals=tokens),
        name=f'dn{tile_off}',
    )(*dus, w1o, w1o, w1r, w1r, w3o, w3o, w3r, w3r, h, g, *z, *bufs)


def copy_kernel(src, dst):
    dst[...] = src[...]


def copy_call(x):
    spec = pl.BlockSpec((512, x.shape[1]), lambda i: (i, 0))
    return pl.pallas_call(
        copy_kernel, grid=(x.shape[0] // 512,), in_specs=[spec], out_specs=spec, out_shape=jax.ShapeDtypeStruct(x.shape, x.dtype),
        cost_estimate=pl.CostEstimate(flops=x.size, bytes_accessed=4 * x.size, transcendentals=0), name='out')(x)


def solution(mesh):
    tok_spec = P(('replica', 'fsdp'), None)
    act_spec = P(None, ('replica', 'fsdp'), None)
    weight_spec = P(None, 'fsdp', None)

    def local_step(block_in, grad_out, w_up, w_lin, w_down):
        h, g = block_in[0], grad_out
        own = (w_up[0], w_lin[0], w_down[0])
        half, ff = own[0].shape
        fh = ff // 2
        units = CHUNKS[1][2]
        rest = fh // UNIT - units

        n, *recv = norm_call(h, own)
        bufs = tuple(chunk_call(0, n, g, own, tuple(recv), (), 0, 0, 0))
        *bufs, w1r, w3r, _, full = chunk_call(1, n, g, own, tuple(recv), bufs, CHUNKS[0][0], units, 0)
        dh, part = dn_call(2, bufs[:4], own[0], w1r, own[1], w3r, h, g, bufs[4:], (), 0, h.shape[0] // 512, rest, units)
        part = lax.all_gather(part, 'replica', axis=0, tiled=True).reshape(4, rest, *part.shape[1:])
        outs = place_call(full, (), (), half, fh, 0, 'place0')
        dh = copy_call(dh)
        outs = place_call(part, outs, (dh,), half, fh, units, 'place1')
        return outs[0][None], outs[1][None], outs[2][None], dh

    return jax.shard_map(local_step, mesh=mesh, in_specs=(act_spec, tok_spec, weight_spec, weight_spec, weight_spec), out_specs=(weight_spec, weight_spec, weight_spec, tok_spec), check_vma=False)
```

```python
import functools

import jax
import jax.numpy as jnp
from jax import lax
from jax.experimental import pallas as pl
from jax.experimental.pallas import tpu as pltpu
from jax.sharding import PartitionSpec as P

NORM_EPS = 1e-5
BF16 = jnp.bfloat16
F32 = jnp.float32
VMEM_LIMIT = 62 * 1024 * 1024
UNIT = 32
SLOTS = 4
F_SLOTS = 8
G_SLOTS = 16
STEP = 256
MAIN = (72, 16)
TAILS = ((4, 4, 28), (4, 8, 0))
FINISH = 3
EARLY = 768
TILE = 512
ANY = pl.BlockSpec(memory_space=pl.ANY)
MESH = pl.DeviceIdType.MESH


def SMALL():
    global STEP, MAIN, TAILS, EARLY, FINISH
    STEP, MAIN, TAILS, EARLY, FINISH = 128, (8, 4), ((1, 4, 8), (1, 8, 0)), 384, 1


def dot_nn(a, b):
    return lax.dot_general(a, b, (((1,), (0,)), ((), ())), preferred_element_type=F32)


def dot_nt(a, b):
    return lax.dot_general(a, b, (((1,), (1,)), ((), ())), preferred_element_type=F32)


def dot_tn(a, b):
    return lax.dot_general(a, b, (((0,), (0,)), ((), ())), preferred_element_type=F32)


def exchange(w1o, w3o, w2o, into, lo, hi, send_sem, recv_sem):
    r, k, _, _ = position()
    f_half = w1o.shape[1] // 2
    pairs = [(src.at[:, pl.ds(p * f_half + lo, hi - lo)], dst.at[:, pl.ds(p * f_half + lo, hi - lo)])
             for src, dst in ((w1o, into[0]), (w3o, into[1])) for p in range(2)]
    pairs.append((w2o.at[pl.ds(lo, hi - lo), :], into[2].at[pl.ds(lo, hi - lo), :]))
    return [pltpu.make_async_remote_copy(
        src_ref=src, dst_ref=dst, send_sem=send_sem.at[num], recv_sem=recv_sem.at[num],
        device_id=(r, 1 - k), device_id_type=MESH) for num, (src, dst) in enumerate(pairs)]


def norm_kernel(n_tiles, h_ref, w1o, w3o, w2o, n_ref, w1r, w3r, w2r, send_sem, recv_sem):
    i = pl.program_id(0)
    r, k, _, _ = position()
    args = (w1o, w3o, w2o, (w1r, w3r, w2r), 0, EARLY, send_sem, recv_sem)

    @pl.when(i == 0)
    def _():
        barrier = pltpu.get_barrier_semaphore()
        pl.semaphore_signal(barrier, inc=1, device_id=(r, 1 - k), device_id_type=MESH)
        pl.semaphore_wait(barrier, 1)
        for copy in exchange(*args):
            copy.start()

    half = h_ref.shape[1] // 2
    h = h_ref[...].astype(F32)
    inv_rms = lax.rsqrt(jnp.mean(h * h, axis=-1, keepdims=True) + NORM_EPS)
    y = (h * inv_rms).astype(BF16)
    first = k == 0
    n_ref[:, :half] = jnp.where(first, y[:, :half], y[:, half:])
    n_ref[:, half:] = jnp.where(first, y[:, half:], y[:, :half])

    @pl.when(i == n_tiles - 1)
    def _():
        for copy in exchange(*args):
            copy.wait()


def norm_call(h, own):
    tokens, dim = h.shape
    tile = 512
    spec = pl.BlockSpec((tile, dim), lambda i: (i, 0))
    return pl.pallas_call(
        functools.partial(norm_kernel, tokens // tile),
        grid=(tokens // tile,),
        in_specs=[spec] + [ANY] * 3,
        out_specs=[spec] + [ANY] * 3,
        scratch_shapes=[pltpu.SemaphoreType.DMA((5,)), pltpu.SemaphoreType.DMA((5,))],
        out_shape=[jax.ShapeDtypeStruct((tokens, dim), BF16)] + [jax.ShapeDtypeStruct(w.shape, BF16) for w in own],
        compiler_params=pltpu.CompilerParams(vmem_limit_bytes=VMEM_LIMIT, collective_id=8, has_side_effects=True),
        cost_estimate=pl.CostEstimate(flops=6 * tokens * dim, bytes_accessed=4 * tokens * dim, transcendentals=tokens),
        name='norm',
    )(h, *own)


def rs_scratch(dim):
    rows = 3 * UNIT
    return [
        pltpu.VMEM((SLOTS, rows, dim), F32),
        pltpu.VMEM((SLOTS, rows, dim), F32),
        pltpu.VMEM((SLOTS, rows, dim // 2), F32),
        pltpu.VMEM((SLOTS, rows, dim // 2), F32),
        pltpu.VMEM((SLOTS, rows, dim // 4), F32),
        pltpu.VMEM((F_SLOTS, rows, dim // 4), F32),
        pltpu.SemaphoreType.DMA((SLOTS, 6)),
        pltpu.SemaphoreType.DMA((SLOTS, 4)),
        pltpu.SemaphoreType.DMA((SLOTS, 4)),
        pltpu.SemaphoreType.DMA((F_SLOTS,)),
        pltpu.SemaphoreType.DMA((G_SLOTS, 6)),
        pltpu.SemaphoreType.DMA((G_SLOTS, 6)),
        pltpu.SemaphoreType.REGULAR((4,)),
    ]


def position():
    r = lax.axis_index('replica')
    k = lax.axis_index('fsdp')
    x, y = lax.rem(r, 2), lax.div(r, 2)
    return r, k, x, y


def enter(step):
    r, k, x, y = position()

    @pl.when(step == 0)
    def _():
        barrier = pltpu.get_barrier_semaphore()
        for peer in ((r, 1 - k), (r + 1 - 2 * x, k), (r + 2 - 4 * y, k)):
            pl.semaphore_signal(barrier, inc=1, device_id=peer, device_id_type=MESH)
        pl.semaphore_wait(barrier, 3)


def ticks(step, begin, n_grid, n_all, n_part, first, z_own, z_in, full, part, scratch):
    own_buf, in_buf, r1, y2, r2, f_buf, load_sem, send_sem, recv_sem, out_sem, g_send, g_recv, credit = scratch
    r, k, x, y = position()
    at_x, at_y = (r + 1 - 2 * x, k), (r + 2 - 4 * y, k)
    dim = own_buf.shape[2]
    quarter, eighth = dim // 4, dim // 8
    n_units = n_all + n_part
    n_ticks = max(n_all + 11, n_units + 7) if n_all else n_units + 7

    def loads(u):
        slot = lax.rem(u, SLOTS)
        row = pl.multiple_of((first + u) * UNIT, UNIT)
        copies = []
        for part in range(3):
            dst = pl.ds(part * UNIT, UNIT)
            copies.append(pltpu.make_async_copy(z_own.at[part, pl.ds(row, UNIT), :], own_buf.at[slot, dst, :], load_sem.at[slot, part]))
            copies.append(pltpu.make_async_copy(z_in.at[part, pl.ds(row, UNIT), :], in_buf.at[slot, dst, :], load_sem.at[slot, 3 + part]))
        return copies

    def lanes(base, index, width):
        return pl.ds(pl.multiple_of(base + index * width, 128), width)

    def first_hop(u):
        slot = lax.rem(u, SLOTS)
        out = []
        for i, (base, index, peer, col) in enumerate(((0, 1 - x, at_x, 0), (dim // 2, 1 - y, at_y, quarter))):
            out.append(pltpu.make_async_remote_copy(
                src_ref=own_buf.at[slot, :, lanes(base, index, quarter)], dst_ref=r1.at[slot, :, pl.ds(col, quarter)],
                send_sem=send_sem.at[slot, i], recv_sem=recv_sem.at[slot, i], device_id=peer, device_id_type=MESH))
        return out

    def second_hop(u):
        slot = lax.rem(u, SLOTS)
        out = []
        for i, (base, index, peer, col) in enumerate(((0, 1 - y, at_y, 0), (quarter, 1 - x, at_x, eighth))):
            out.append(pltpu.make_async_remote_copy(
                src_ref=y2.at[slot, :, lanes(base, index, eighth)], dst_ref=r2.at[slot, :, pl.ds(col, eighth)],
                send_sem=send_sem.at[slot, 2 + i], recv_sem=recv_sem.at[slot, 2 + i], device_id=peer, device_id_type=MESH))
        return out

    def store_all(u):
        slot = lax.rem(u, F_SLOTS)
        return pltpu.make_async_copy(f_buf.at[slot], full.at[r, u], out_sem.at[slot])

    def store_part(u):
        slot = lax.rem(u, F_SLOTS)
        return pltpu.make_async_copy(f_buf.at[slot], part.at[u - n_all], out_sem.at[slot])

    def spread(u, num, src, origin, col, peer):
        slot = lax.rem(u, G_SLOTS)
        return pltpu.make_async_remote_copy(
            src_ref=src, dst_ref=full.at[origin, u, :, pl.ds(col, eighth)], send_sem=g_send.at[slot, num],
            recv_sem=g_recv.at[slot, num], device_id=peer, device_id_type=MESH)

    def third_hop(u):
        slot = lax.rem(u, F_SLOTS)
        return [spread(u, i, f_buf.at[slot, :, pl.ds(col, eighth)], r, col, peer)
                for i, (col, peer) in enumerate(((0, at_y), (eighth, at_x)))]

    def fourth_hop(u):
        slot = lax.rem(u, F_SLOTS)
        return [spread(u, 2 + i, f_buf.at[slot, :, pl.ds(col, eighth)], r, col, peer)
                for i, (col, peer) in enumerate(((0, at_x), (eighth, at_y)))]

    def forward(u):
        return [spread(u, 4 + i, full.at[origin, u, :, pl.ds(col, eighth)], origin, col, peer)
                for i, (origin, col, peer) in enumerate(((at_y[0], 0, at_x), (at_x[0], eighth, at_y)))]

    def stage(tick, lag, fn, lo=0, hi=n_units):
        if lo < hi:
            u = tick - lag

            @pl.when(jnp.logical_and(u >= lo, u < hi))
            def _():
                fn(u, lax.rem(u, SLOTS))

    def do_load(u, slot):
        for copy in loads(u):
            copy.start()

    def do_first(u, slot):
        for copy in loads(u):
            copy.wait()
        own_buf[slot] = own_buf[slot] + in_buf[slot]

        @pl.when(u >= SLOTS)
        def _():
            pl.semaphore_wait(credit.at[0], 1)
            pl.semaphore_wait(credit.at[1], 1)

        for copy in first_hop(u):
            copy.start()

    def do_second(u, slot):
        for copy in first_hop(u):
            copy.wait()
        y2[slot, :, :quarter] = own_buf[slot, :, lanes(0, x, quarter)] + r1[slot, :, :quarter]
        y2[slot, :, quarter:] = own_buf[slot, :, lanes(dim // 2, y, quarter)] + r1[slot, :, quarter:]

        @pl.when(u < n_units - SLOTS)
        def _():
            pl.semaphore_signal(credit.at[0], inc=1, device_id=at_x, device_id_type=MESH)
            pl.semaphore_signal(credit.at[1], inc=1, device_id=at_y, device_id_type=MESH)

        @pl.when(u >= SLOTS)
        def _():
            pl.semaphore_wait(credit.at[2], 1)
            pl.semaphore_wait(credit.at[3], 1)

        for copy in second_hop(u):
            copy.start()

    def do_third(u, slot):
        for copy in second_hop(u):
            copy.wait()
        f_slot = lax.rem(u, F_SLOTS)
        f_buf[f_slot, :, :eighth] = y2[slot, :, lanes(0, y, eighth)] + r2[slot, :, :eighth]
        f_buf[f_slot, :, eighth:] = y2[slot, :, lanes(quarter, x, eighth)] + r2[slot, :, eighth:]

        @pl.when(u < n_units - SLOTS)
        def _():
            pl.semaphore_signal(credit.at[2], inc=1, device_id=at_y, device_id_type=MESH)
            pl.semaphore_signal(credit.at[3], inc=1, device_id=at_x, device_id_type=MESH)

        if n_all:
            @pl.when(u < n_all)
            def _():
                store_all(u).start()
                for copy in third_hop(u) + fourth_hop(u):
                    copy.start()

        if n_part:
            @pl.when(u >= n_all)
            def _():
                store_part(u).start()

    def do_forward(u, slot):
        for copy in third_hop(u):
            copy.wait()
        for copy in forward(u):
            copy.start()

    def end_all(u, slot):
        store_all(u).wait()
        for copy in fourth_hop(u) + forward(u):
            copy.wait()

    def end_part(u, slot):
        store_part(u).wait()

    def tick(t, carry):
        stage(t, 10, end_all, 0, n_all)
        stage(t, 7, do_forward, 0, n_all)
        stage(t, 6, end_part, n_all, n_units)
        stage(t, 5, do_third)
        stage(t, 3, do_second)
        stage(t, 1, do_first)
        stage(t, 0, do_load)
        return carry

    spread_steps = n_grid - FINISH - begin
    lead = n_units + 1
    late = step // (n_grid - FINISH)

    def bound(at):
        here = ((at - begin) * lead) // spread_steps
        there = lead + ((at - (n_grid - FINISH)) * (n_ticks - lead)) // FINISH
        return (1 - late) * here + late * there

    @pl.when(step >= begin)
    def _():
        lax.fori_loop(bound(step), bound(step + 1), tick, 0)


def chunk_kernel(sh, n_steps, n_tiles, n_ref, g_ref, w1o, w3o, w2o, *rest):
    du_0, du_1, dv_0, dv_1, z_own, z_in, w1r, w3r, w2r, full, part = rest[3:14]
    w13, w2c, acc13, acc2, w_sem, out_sem, d_send, d_recv, p_send, p_recv = rest[14:24]
    half = w1o.shape[0]
    f_half = w1o.shape[1] // 2
    wide = 2 * sh
    j = pl.program_id(0)
    i = pl.program_id(1)
    slot = lax.rem(j, 2)
    r, k, _, _ = position()
    own_row = pl.multiple_of(k * sh, 128)
    oth_row = pl.multiple_of((1 - k) * sh, 128)
    enter(j * n_tiles + i)
    ticks(j * n_tiles + i, n_tiles + 1, n_steps * n_tiles, *MAIN, 0, z_own, z_in, full, part, rest[24:])

    def fetches(step, buf):
        copies = []

        def add(src, dst):
            copies.append(pltpu.make_async_copy(src, dst, w_sem.at[buf, len(copies)]))

        at = pl.multiple_of(step * sh, 128)
        for own_src, oth_src, col in ((w1o, w1r, 0), (w3o, w3r, wide)):
            for src, row in ((own_src, 0), (oth_src, half)):
                for p in range(2):
                    add(src.at[:, pl.ds(p * f_half + at, sh)], w13.at[buf, pl.ds(row, half), pl.ds(col + p * sh, sh)])
        for src, row in ((w2o, own_row), (w2r, oth_row)):
            add(src.at[pl.ds(at, sh), :], w2c.at[buf, pl.ds(row, sh), :])
        return copies

    def drains(step):
        row = pl.multiple_of(step * sh, 128)
        local, remote = [], []

        def add(keep, send, part, lanes):
            num = len(local)
            local.append(pltpu.make_async_copy(keep, z_own.at[part, pl.ds(row, sh), lanes], out_sem.at[num]))
            remote.append(pltpu.make_async_remote_copy(
                src_ref=send, dst_ref=z_in.at[part, pl.ds(row, sh), lanes], send_sem=d_send.at[num], recv_sem=d_recv.at[step, num],
                device_id=(r, 1 - k), device_id_type=MESH))

        for part in range(2):
            for p in range(2):
                src = pl.ds(part * wide + p * sh, sh)
                add(acc13.at[src, pl.ds(0, half)], acc13.at[src, pl.ds(half, half)], part, pl.ds(p * half, half))
        add(acc2.at[pl.ds(own_row, sh), :], acc2.at[pl.ds(oth_row, sh), :], 2, pl.ds(0, 2 * half))
        return local, remote

    def finish(step):
        local, remote = drains(step)
        for copy in local:
            copy.wait()
        for copy in remote:
            copy.wait()

    args = (w1o, w3o, w2o, (w1r, w3r, w2r), EARLY, f_half, p_send, p_recv)

    @pl.when(jnp.logical_and(i == 0, j == 0))
    def _():
        for copy in exchange(*args):
            copy.start()

    @pl.when(jnp.logical_and(i == 0, j == EARLY // sh - 1))
    def _():
        for copy in exchange(*args):
            copy.wait()

    @pl.when(i == 0)
    def _():
        @pl.when(j == 0)
        def _():
            for copy in fetches(0, 0):
                copy.start()

        for copy in fetches(j, slot):
            copy.wait()

        @pl.when(j + 1 < n_steps)
        def _():
            for copy in fetches(j + 1, 1 - slot):
                copy.start()

    n = n_ref[...]
    g = g_ref[...]
    uv = dot_nn(n, w13[slot])
    da = dot_nt(g, w2c[slot])
    u = uv[:, :wide]
    v = uv[:, wide:]
    sig = jax.nn.sigmoid(u)
    up_act = u * sig
    act = (up_act * v).astype(BF16)
    du = (da * v * sig * (1.0 + u * (1.0 - sig))).astype(BF16)
    dv = (da * up_act).astype(BF16)
    du_0[...] = du[:, :sh]
    du_1[...] = du[:, sh:]
    dv_0[...] = dv[:, :sh]
    dv_1[...] = dv[:, sh:]

    @pl.when(jnp.logical_and(i == 0, j > 0))
    def _():
        finish(j - 1)

    @pl.when(i == 0)
    def _():
        acc13[...] = jnp.zeros_like(acc13)
        acc2[...] = jnp.zeros_like(acc2)

    acc2[...] += dot_tn(act, g)
    acc13[...] += dot_tn(jnp.concatenate([du, dv], axis=1), n)

    @pl.when(i == n_tiles - 1)
    def _():
        local, remote = drains(j)
        for copy in remote + local:
            copy.start()

        @pl.when(j == n_steps - 1)
        def _():
            finish(j)


def sums(n_all, n_part, dim):
    block = (3 * UNIT, dim // 4)
    return ([jax.ShapeDtypeStruct((4, n_all, *block), F32)] if n_all else []) + ([jax.ShapeDtypeStruct((n_part, *block), F32)] if n_part else [])


def chunk_call(n, g, own, recv):
    tokens, dim = n.shape
    f_half = own[0].shape[1] // 2
    sh, tile = STEP, TILE
    n_steps, n_tiles = f_half // sh, tokens // tile
    tile_spec = pl.BlockSpec((tile, sh), lambda j, i: (i, j))
    row_spec = pl.BlockSpec((tile, dim), lambda j, i: (i, 0))
    big = jax.ShapeDtypeStruct((tokens, f_half), BF16)
    z = jax.ShapeDtypeStruct((3, f_half, dim), F32)
    return pl.pallas_call(
        functools.partial(chunk_kernel, sh, n_steps, n_tiles),
        grid=(n_steps, n_tiles),
        in_specs=[row_spec, row_spec] + [ANY] * 6,
        out_specs=[tile_spec] * 4 + [ANY] * 7,
        scratch_shapes=[
            pltpu.VMEM((2, dim, 4 * sh), BF16),
            pltpu.VMEM((2, 2 * sh, dim), BF16),
            pltpu.VMEM((4 * sh, dim), F32),
            pltpu.VMEM((2 * sh, dim), F32),
            pltpu.SemaphoreType.DMA((2, 10)),
            pltpu.SemaphoreType.DMA((5,)),
            pltpu.SemaphoreType.DMA((5,)),
            pltpu.SemaphoreType.DMA((n_steps, 5)),
            pltpu.SemaphoreType.DMA((5,)),
            pltpu.SemaphoreType.DMA((5,)),
        ] + rs_scratch(dim),
        out_shape=[big] * 4 + [z] * 2 + [jax.ShapeDtypeStruct(w.shape, BF16) for w in own] + sums(*MAIN, dim),
        input_output_aliases={5: 6, 6: 7, 7: 8},
        compiler_params=pltpu.CompilerParams(
            vmem_limit_bytes=VMEM_LIMIT, dimension_semantics=('arbitrary', 'arbitrary'), collective_id=0, has_side_effects=True),
        cost_estimate=pl.CostEstimate(flops=24 * tokens * dim * f_half, bytes_accessed=n_steps * 4 * tokens * dim + 24 * dim * f_half, transcendentals=tokens * 2 * f_half),
        name='chunks',
    )(n, g, *own, *recv)


def place_kernel(n_any, z, *rest):
    out1, out3, out2 = rest[n_any:]
    p = pl.program_id(1)
    _, n_units, _, eighth = z.shape
    rows = n_units * UNIT
    for r in range(4):
        x, y = r % 2, r // 2
        for half, index in ((0, 2 * x + y), (1, 2 * y + x)):
            @pl.when(p == half)
            def _():
                at = pl.ds(index * eighth, eighth)
                out1[at, :] = z[r, :, :UNIT, :].reshape(rows, eighth).T
                out3[at, :] = z[r, :, UNIT:2 * UNIT, :].reshape(rows, eighth).T
                out2[:, at] = z[r, :, 2 * UNIT:, :].reshape(rows, eighth)


def place_call(z, outs, after, half, f_half, first_unit, name):
    dim = 2 * half
    units = z.shape[1]
    group = 8 if units % 8 == 0 and first_unit % 8 == 0 else 4
    sb = group * UNIT
    first, f_blocks = first_unit // group, f_half // sb
    n_alias = len(outs)
    side = jax.ShapeDtypeStruct((half, 2 * f_half), F32)
    side_spec = pl.BlockSpec((half, sb), lambda j, p: (0, p * f_blocks + first + j))
    return pl.pallas_call(
        functools.partial(place_kernel, n_alias + len(after)),
        grid=(units // group, 2),
        in_specs=[pl.BlockSpec((4, group, 3 * UNIT, dim // 8), lambda j, p: (0, j, 0, p))] + [ANY] * (n_alias + len(after)),
        out_specs=[side_spec, side_spec, pl.BlockSpec((sb, half), lambda j, p: (first + j, p))],
        out_shape=[side, side, jax.ShapeDtypeStruct((f_half, dim), F32)],
        input_output_aliases={1 + a: a for a in range(n_alias)},
        compiler_params=pltpu.CompilerParams(vmem_limit_bytes=VMEM_LIMIT, dimension_semantics=('arbitrary', 'arbitrary')),
        cost_estimate=pl.CostEstimate(flops=3 * units * UNIT * dim, bytes_accessed=24 * units * UNIT * dim, transcendentals=0),
        name=name,
    )(z, *outs, *after)


def dn_kernel(n_tiles, n_steps, n_alias, n_all, n_part, first_unit, *refs):
    (du_0, du_1, dv_0, dv_1, w1o_0, w1o_1, w1r_0, w1r_1, w3o_0, w3o_1, w3r_0, w3r_1, h_ref, g_ref, z_own, z_in) = refs[:16]
    rest = refs[16 + n_alias:]
    out_ref = rest[0]
    full = rest[1] if n_all else None
    n_out = 1 + bool(n_all) + bool(n_part)
    part = rest[n_out - 1] if n_part else None
    acc_own, acc_oth = rest[n_out:n_out + 2]
    f = pl.program_id(1)
    half = acc_own.shape[1]
    step = pl.program_id(0) * n_steps + f
    enter(step)
    ticks(step, 0, n_tiles * n_steps, n_all, n_part, first_unit, z_own, z_in, full, part, rest[n_out + 2:])

    @pl.when(f == 0)
    def _():
        acc_own[...] = jnp.zeros_like(acc_own)
        acc_oth[...] = jnp.zeros_like(acc_oth)

    acc_own[...] += (dot_nt(du_0[...], w1o_0[...]) + dot_nt(du_1[...], w1o_1[...])
                     + dot_nt(dv_0[...], w3o_0[...]) + dot_nt(dv_1[...], w3o_1[...]))
    acc_oth[...] += (dot_nt(du_0[...], w1r_0[...]) + dot_nt(du_1[...], w1r_1[...])
                     + dot_nt(dv_0[...], w3r_0[...]) + dot_nt(dv_1[...], w3r_1[...]))

    @pl.when(f == n_steps - 1)
    def _():
        rows = 256
        first = lax.axis_index('fsdp') == 0
        for t in range(out_ref.shape[0] // rows):
            sl = pl.ds(t * rows, rows)
            h = h_ref[sl, :].astype(F32)
            inv_rms = lax.rsqrt(jnp.mean(h * h, axis=-1, keepdims=True) + NORM_EPS)
            y = h * inv_rms
            own, oth = acc_own[sl, :], acc_oth[sl, :]
            d = jnp.concatenate([jnp.where(first, own, oth), jnp.where(first, oth, own)], axis=1)
            mean = jnp.mean(d * y, axis=-1, keepdims=True)
            out_ref[sl, :] = (g_ref[sl, :].astype(F32) + inv_rms * (d - y * mean)).astype(BF16)


def dn_call(c, dus, w1o, w1r, w3o, w3r, h, g, z, bufs, tile_off, n_tiles, n_all, n_part, first_unit):
    tokens, dim = h.shape
    half = dim // 2
    tile, fb = 512, 512
    n_steps = dus[0].shape[1] // fb
    d_spec = pl.BlockSpec((tile, fb), lambda i, f: (tile_off + i, f))
    w_0 = pl.BlockSpec((half, fb), lambda i, f: (0, f))
    w_1 = pl.BlockSpec((half, fb), lambda i, f: (0, n_steps + f))
    row_spec = pl.BlockSpec((tile, dim), lambda i, f: (tile_off + i, 0))
    n_alias = len(bufs)
    out = sums(n_all, n_part, dim)
    return pl.pallas_call(
        functools.partial(dn_kernel, n_tiles, n_steps, n_alias, n_all, n_part, first_unit),
        grid=(n_tiles, n_steps),
        in_specs=[d_spec] * 4 + [w_0, w_1] * 4 + [row_spec, row_spec] + [ANY] * (2 + n_alias),
        out_specs=[row_spec] + [ANY] * len(out),
        scratch_shapes=[pltpu.VMEM((tile, half), F32), pltpu.VMEM((tile, half), F32)] + rs_scratch(dim),
        out_shape=[jax.ShapeDtypeStruct((tokens, dim), BF16)] + out,
        input_output_aliases={16 + a: a for a in range(n_alias)},
        compiler_params=pltpu.CompilerParams(vmem_limit_bytes=VMEM_LIMIT, dimension_semantics=('arbitrary', 'arbitrary'), collective_id=c, has_side_effects=True),
        cost_estimate=pl.CostEstimate(flops=8 * n_tiles * tile * dim * n_steps * fb, bytes_accessed=8 * n_tiles * tile * n_steps * fb + 8 * n_tiles * dim * n_steps * fb, transcendentals=tokens),
        name=f'dn{tile_off}',
    )(*dus, w1o, w1o, w1r, w1r, w3o, w3o, w3r, w3r, h, g, *z, *bufs)


def copy_kernel(src, dst):
    dst[...] = src[...]


def copy_call(x):
    spec = pl.BlockSpec((512, x.shape[1]), lambda i: (i, 0))
    return pl.pallas_call(
        copy_kernel, grid=(x.shape[0] // 512,), in_specs=[spec], out_specs=spec, out_shape=jax.ShapeDtypeStruct(x.shape, x.dtype),
        cost_estimate=pl.CostEstimate(flops=x.size, bytes_accessed=4 * x.size, transcendentals=0), name='out')(x)


def solution(mesh):
    tok_spec = P(('replica', 'fsdp'), None)
    act_spec = P(None, ('replica', 'fsdp'), None)
    weight_spec = P(None, 'fsdp', None)

    def local_step(block_in, grad_out, w_up, w_lin, w_down):
        h, g = block_in[0], grad_out
        own = (w_up[0], w_lin[0], w_down[0])
        half, ff = own[0].shape
        fh = ff // 2

        def gather(part):
            return lax.all_gather(part, 'replica', axis=0, tiled=True).reshape(4, *part.shape)

        n, *recv = norm_call(h, own)
        *dus, z_own, z_in, w1r, w3r, _, full, part = chunk_call(n, g, own, recv)
        placed = [(0, full)]
        late = [(MAIN[0], gather(part))]
        first, tile_off = sum(MAIN), 0
        dh = ()
        for c, (tiles, n_all, n_part) in enumerate(TAILS):
            dh, *res = dn_call(1 + c, dus, own[0], w1r, own[1], w3r, h, g, (z_own, z_in), dh, tile_off, tiles, n_all, n_part, first)
            dh = (dh,)
            if n_all:
                placed.append((first, res[0]))
            if n_part:
                late.append((first + n_all, gather(res[-1])))
            tile_off += tiles
            first += n_all + n_part
        dh = copy_call(dh[0])
        outs = ()
        jobs = placed + late
        for i, (unit, sums_of) in enumerate(jobs):
            after = (dh,) if i == len(jobs) - 1 else ()
            outs = tuple(place_call(sums_of, outs, after, half, fh, unit, f'place{unit}'))
        return outs[0][None], outs[1][None], outs[2][None], dh

    return jax.shard_map(local_step, mesh=mesh, in_specs=(act_spec, tok_spec, weight_spec, weight_spec, weight_spec), out_specs=(weight_spec, weight_spec, weight_spec, tok_spec), check_vma=False)
```

```python
import functools

import jax
import jax.numpy as jnp
from jax import lax
from jax.experimental import pallas as pl
from jax.experimental.pallas import tpu as pltpu
from jax.sharding import PartitionSpec as P

NORM_EPS = 1e-5
BF16 = jnp.bfloat16
F32 = jnp.float32
VMEM_LIMIT = 62 * 1024 * 1024
UNIT = 32
SLOTS = 4
F_SLOTS = 8
G_SLOTS = 16
STEP = 256
MAIN = (84, 8)
TAILS = ((8, 24, 12),)
FINISH = 3
EARLY = (512, 2048)
TILE = 512
ANY = pl.BlockSpec(memory_space=pl.ANY)
MESH = pl.DeviceIdType.MESH


def SMALL():
    global STEP, MAIN, TAILS, EARLY, FINISH
    STEP, MAIN, TAILS, EARLY, FINISH = 128, (8, 4), ((2, 8, 12),), (256, 512), 1


def dot_nn(a, b):
    return lax.dot_general(a, b, (((1,), (0,)), ((), ())), preferred_element_type=F32)


def dot_nt(a, b):
    return lax.dot_general(a, b, (((1,), (1,)), ((), ())), preferred_element_type=F32)


def dot_tn(a, b):
    return lax.dot_general(a, b, (((0,), (0,)), ((), ())), preferred_element_type=F32)


def exchange(w1o, w3o, w2o, into, lo, hi, send_sem, recv_sem):
    r, k, _, _ = position()
    f_half = w1o.shape[1] // 2
    pairs = [(src.at[:, pl.ds(p * f_half + lo, hi - lo)], dst.at[:, pl.ds(p * f_half + lo, hi - lo)])
             for src, dst in ((w1o, into[0]), (w3o, into[1])) for p in range(2)]
    pairs.append((w2o.at[pl.ds(lo, hi - lo), :], into[2].at[pl.ds(lo, hi - lo), :]))
    return [pltpu.make_async_remote_copy(
        src_ref=src, dst_ref=dst, send_sem=send_sem.at[num], recv_sem=recv_sem.at[num],
        device_id=(r, 1 - k), device_id_type=MESH) for num, (src, dst) in enumerate(pairs)]


def norm_kernel(n_tiles, h_ref, w1o, w3o, w2o, n_ref, w1r, w3r, w2r, send_sem, recv_sem):
    i = pl.program_id(0)
    r, k, _, _ = position()
    args = (w1o, w3o, w2o, (w1r, w3r, w2r), 0, EARLY[0], send_sem, recv_sem)

    @pl.when(i == 0)
    def _():
        barrier = pltpu.get_barrier_semaphore()
        pl.semaphore_signal(barrier, inc=1, device_id=(r, 1 - k), device_id_type=MESH)
        pl.semaphore_wait(barrier, 1)
        for copy in exchange(*args):
            copy.start()

    half = h_ref.shape[1] // 2
    h = h_ref[...].astype(F32)
    inv_rms = lax.rsqrt(jnp.mean(h * h, axis=-1, keepdims=True) + NORM_EPS)
    y = (h * inv_rms).astype(BF16)
    first = k == 0
    n_ref[:, :half] = jnp.where(first, y[:, :half], y[:, half:])
    n_ref[:, half:] = jnp.where(first, y[:, half:], y[:, :half])

    @pl.when(i == n_tiles - 1)
    def _():
        for copy in exchange(*args):
            copy.wait()


def norm_call(h, own):
    tokens, dim = h.shape
    tile = 512
    spec = pl.BlockSpec((tile, dim), lambda i: (i, 0))
    return pl.pallas_call(
        functools.partial(norm_kernel, tokens // tile),
        grid=(tokens // tile,),
        in_specs=[spec] + [ANY] * 3,
        out_specs=[spec] + [ANY] * 3,
        scratch_shapes=[pltpu.SemaphoreType.DMA((5,)), pltpu.SemaphoreType.DMA((5,))],
        out_shape=[jax.ShapeDtypeStruct((tokens, dim), BF16)] + [jax.ShapeDtypeStruct(w.shape, BF16) for w in own],
        compiler_params=pltpu.CompilerParams(vmem_limit_bytes=VMEM_LIMIT, collective_id=8, has_side_effects=True),
        cost_estimate=pl.CostEstimate(flops=6 * tokens * dim, bytes_accessed=4 * tokens * dim, transcendentals=tokens),
        name='norm',
    )(h, *own)


def rs_scratch(dim):
    rows = 3 * UNIT
    return [
        pltpu.VMEM((SLOTS, rows, dim), F32),
        pltpu.VMEM((SLOTS, rows, dim), F32),
        pltpu.VMEM((SLOTS, rows, dim // 2), F32),
        pltpu.VMEM((SLOTS, rows, dim // 2), F32),
        pltpu.VMEM((SLOTS, rows, dim // 4), F32),
        pltpu.VMEM((F_SLOTS, rows, dim // 4), F32),
        pltpu.SemaphoreType.DMA((SLOTS, 6)),
        pltpu.SemaphoreType.DMA((SLOTS, 4)),
        pltpu.SemaphoreType.DMA((SLOTS, 4)),
        pltpu.SemaphoreType.DMA((F_SLOTS,)),
        pltpu.SemaphoreType.DMA((G_SLOTS, 6)),
        pltpu.SemaphoreType.DMA((G_SLOTS, 6)),
        pltpu.SemaphoreType.REGULAR((4,)),
    ]


def position():
    r = lax.axis_index('replica')
    k = lax.axis_index('fsdp')
    x, y = lax.rem(r, 2), lax.div(r, 2)
    return r, k, x, y


def enter(step):
    r, k, x, y = position()

    @pl.when(step == 0)
    def _():
        barrier = pltpu.get_barrier_semaphore()
        for peer in ((r, 1 - k), (r + 1 - 2 * x, k), (r + 2 - 4 * y, k)):
            pl.semaphore_signal(barrier, inc=1, device_id=peer, device_id_type=MESH)
        pl.semaphore_wait(barrier, 3)


def ticks(step, begin, n_lead, n_grid, n_all, n_part, first, z_own, z_in, full, part, scratch):
    own_buf, in_buf, r1, y2, r2, f_buf, load_sem, send_sem, recv_sem, out_sem, g_send, g_recv, credit = scratch
    r, k, x, y = position()
    at_x, at_y = (r + 1 - 2 * x, k), (r + 2 - 4 * y, k)
    dim = own_buf.shape[2]
    quarter, eighth = dim // 4, dim // 8
    n_units = n_all + n_part
    n_ticks = max(n_all + 11, n_units + 7) if n_all else n_units + 7

    def loads(u):
        slot = lax.rem(u, SLOTS)
        row = pl.multiple_of((first + u) * UNIT, UNIT)
        copies = []
        for part in range(3):
            dst = pl.ds(part * UNIT, UNIT)
            copies.append(pltpu.make_async_copy(z_own.at[part, pl.ds(row, UNIT), :], own_buf.at[slot, dst, :], load_sem.at[slot, part]))
            copies.append(pltpu.make_async_copy(z_in.at[part, pl.ds(row, UNIT), :], in_buf.at[slot, dst, :], load_sem.at[slot, 3 + part]))
        return copies

    def lanes(base, index, width):
        return pl.ds(pl.multiple_of(base + index * width, 128), width)

    def first_hop(u):
        slot = lax.rem(u, SLOTS)
        out = []
        for i, (base, index, peer, col) in enumerate(((0, 1 - x, at_x, 0), (dim // 2, 1 - y, at_y, quarter))):
            out.append(pltpu.make_async_remote_copy(
                src_ref=own_buf.at[slot, :, lanes(base, index, quarter)], dst_ref=r1.at[slot, :, pl.ds(col, quarter)],
                send_sem=send_sem.at[slot, i], recv_sem=recv_sem.at[slot, i], device_id=peer, device_id_type=MESH))
        return out

    def second_hop(u):
        slot = lax.rem(u, SLOTS)
        out = []
        for i, (base, index, peer, col) in enumerate(((0, 1 - y, at_y, 0), (quarter, 1 - x, at_x, eighth))):
            out.append(pltpu.make_async_remote_copy(
                src_ref=y2.at[slot, :, lanes(base, index, eighth)], dst_ref=r2.at[slot, :, pl.ds(col, eighth)],
                send_sem=send_sem.at[slot, 2 + i], recv_sem=recv_sem.at[slot, 2 + i], device_id=peer, device_id_type=MESH))
        return out

    def store_all(u):
        slot = lax.rem(u, F_SLOTS)
        return pltpu.make_async_copy(f_buf.at[slot], full.at[r, u], out_sem.at[slot])

    def store_part(u):
        slot = lax.rem(u, F_SLOTS)
        return pltpu.make_async_copy(f_buf.at[slot], part.at[u - n_all], out_sem.at[slot])

    def spread(u, num, src, origin, col, peer):
        slot = lax.rem(u, G_SLOTS)
        return pltpu.make_async_remote_copy(
            src_ref=src, dst_ref=full.at[origin, u, :, pl.ds(col, eighth)], send_sem=g_send.at[slot, num],
            recv_sem=g_recv.at[slot, num], device_id=peer, device_id_type=MESH)

    def third_hop(u):
        slot = lax.rem(u, F_SLOTS)
        return [spread(u, i, f_buf.at[slot, :, pl.ds(col, eighth)], r, col, peer)
                for i, (col, peer) in enumerate(((0, at_y), (eighth, at_x)))]

    def fourth_hop(u):
        slot = lax.rem(u, F_SLOTS)
        return [spread(u, 2 + i, f_buf.at[slot, :, pl.ds(col, eighth)], r, col, peer)
                for i, (col, peer) in enumerate(((0, at_x), (eighth, at_y)))]

    def forward(u):
        return [spread(u, 4 + i, full.at[origin, u, :, pl.ds(col, eighth)], origin, col, peer)
                for i, (origin, col, peer) in enumerate(((at_y[0], 0, at_x), (at_x[0], eighth, at_y)))]

    def stage(tick, lag, fn, lo=0, hi=n_units):
        if lo < hi:
            u = tick - lag

            @pl.when(jnp.logical_and(u >= lo, u < hi))
            def _():
                fn(u, lax.rem(u, SLOTS))

    def do_load(u, slot):
        for copy in loads(u):
            copy.start()

    def do_first(u, slot):
        for copy in loads(u):
            copy.wait()
        own_buf[slot] = own_buf[slot] + in_buf[slot]

        @pl.when(u >= SLOTS)
        def _():
            pl.semaphore_wait(credit.at[0], 1)
            pl.semaphore_wait(credit.at[1], 1)

        for copy in first_hop(u):
            copy.start()

    def do_second(u, slot):
        for copy in first_hop(u):
            copy.wait()
        y2[slot, :, :quarter] = own_buf[slot, :, lanes(0, x, quarter)] + r1[slot, :, :quarter]
        y2[slot, :, quarter:] = own_buf[slot, :, lanes(dim // 2, y, quarter)] + r1[slot, :, quarter:]

        @pl.when(u < n_units - SLOTS)
        def _():
            pl.semaphore_signal(credit.at[0], inc=1, device_id=at_x, device_id_type=MESH)
            pl.semaphore_signal(credit.at[1], inc=1, device_id=at_y, device_id_type=MESH)

        @pl.when(u >= SLOTS)
        def _():
            pl.semaphore_wait(credit.at[2], 1)
            pl.semaphore_wait(credit.at[3], 1)

        for copy in second_hop(u):
            copy.start()

    def do_third(u, slot):
        for copy in second_hop(u):
            copy.wait()
        f_slot = lax.rem(u, F_SLOTS)
        f_buf[f_slot, :, :eighth] = y2[slot, :, lanes(0, y, eighth)] + r2[slot, :, :eighth]
        f_buf[f_slot, :, eighth:] = y2[slot, :, lanes(quarter, x, eighth)] + r2[slot, :, eighth:]

        @pl.when(u < n_units - SLOTS)
        def _():
            pl.semaphore_signal(credit.at[2], inc=1, device_id=at_y, device_id_type=MESH)
            pl.semaphore_signal(credit.at[3], inc=1, device_id=at_x, device_id_type=MESH)

        if n_all:
            @pl.when(u < n_all)
            def _():
                store_all(u).start()
                for copy in third_hop(u) + fourth_hop(u):
                    copy.start()

        if n_part:
            @pl.when(u >= n_all)
            def _():
                store_part(u).start()

    def do_forward(u, slot):
        for copy in third_hop(u):
            copy.wait()
        for copy in forward(u):
            copy.start()

    def end_all(u, slot):
        store_all(u).wait()
        for copy in fourth_hop(u) + forward(u):
            copy.wait()

    def end_part(u, slot):
        store_part(u).wait()

    def tick(t, carry):
        stage(t, 10, end_all, 0, n_all)
        stage(t, 7, do_forward, 0, n_all)
        stage(t, 6, end_part, n_all, n_units)
        stage(t, 5, do_third)
        stage(t, 3, do_second)
        stage(t, 1, do_first)
        stage(t, 0, do_load)
        return carry

    spread_steps = n_grid - FINISH - begin
    lead = n_lead + 1
    late = step // (n_grid - FINISH)

    def bound(at):
        here = ((at - begin) * lead) // spread_steps
        there = lead + ((at - (n_grid - FINISH)) * (n_ticks - lead)) // FINISH
        return (1 - late) * here + late * there

    @pl.when(step >= begin)
    def _():
        lax.fori_loop(bound(step), bound(step + 1), tick, 0)


def chunk_kernel(sh, n_steps, n_tiles, n_ref, g_ref, w1o, w3o, w2o, *rest):
    du_0, du_1, dv_0, dv_1, z_own, z_in, w1r, w3r, w2r, full, part = rest[3:14]
    w13, w2c, acc13, acc2, w_sem, out_sem, d_send, d_recv, p_send, p_recv = rest[14:24]
    half = w1o.shape[0]
    f_half = w1o.shape[1] // 2
    wide = 2 * sh
    j = pl.program_id(0)
    i = pl.program_id(1)
    slot = lax.rem(j, 2)
    r, k, _, _ = position()
    own_row = pl.multiple_of(k * sh, 128)
    oth_row = pl.multiple_of((1 - k) * sh, 128)
    enter(j * n_tiles + i)
    def fetches(step, buf):
        copies = []

        def add(src, dst):
            copies.append(pltpu.make_async_copy(src, dst, w_sem.at[buf, len(copies)]))

        at = pl.multiple_of(step * sh, 128)
        for own_src, oth_src, col in ((w1o, w1r, 0), (w3o, w3r, wide)):
            for src, row in ((own_src, 0), (oth_src, half)):
                for p in range(2):
                    add(src.at[:, pl.ds(p * f_half + at, sh)], w13.at[buf, pl.ds(row, half), pl.ds(col + p * sh, sh)])
        for src, row in ((w2o, own_row), (w2r, oth_row)):
            add(src.at[pl.ds(at, sh), :], w2c.at[buf, pl.ds(row, sh), :])
        return copies

    def drains(step):
        row = pl.multiple_of(step * sh, 128)
        local, remote = [], []

        def add(keep, send, part, lanes):
            num = len(local)
            local.append(pltpu.make_async_copy(keep, z_own.at[part, pl.ds(row, sh), lanes], out_sem.at[num]))
            remote.append(pltpu.make_async_remote_copy(
                src_ref=send, dst_ref=z_in.at[part, pl.ds(row, sh), lanes], send_sem=d_send.at[num], recv_sem=d_recv.at[step, num],
                device_id=(r, 1 - k), device_id_type=MESH))

        for part in range(2):
            for p in range(2):
                src = pl.ds(part * wide + p * sh, sh)
                add(acc13.at[src, pl.ds(0, half)], acc13.at[src, pl.ds(half, half)], part, pl.ds(p * half, half))
        add(acc2.at[pl.ds(own_row, sh), :], acc2.at[pl.ds(oth_row, sh), :], 2, pl.ds(0, 2 * half))
        return local, remote

    def finish(step):
        local, remote = drains(step)
        for copy in local:
            copy.wait()
        for copy in remote:
            copy.wait()

    for num, (lo, hi, at) in enumerate(((*EARLY, (0, 0)), (EARLY[1], f_half, (1, n_tiles // 2)))):
        args = (w1o, w3o, w2o, (w1r, w3r, w2r), lo, hi, p_send.at[num], p_recv.at[num])

        @pl.when(jnp.logical_and(j == at[0], i == at[1]))
        def _():
            for copy in exchange(*args):
                copy.start()

        @pl.when(jnp.logical_and(j == lo // sh - 1, i == 0))
        def _():
            for copy in exchange(*args):
                copy.wait()

    @pl.when(i == 0)
    def _():
        @pl.when(j == 0)
        def _():
            for copy in fetches(0, 0):
                copy.start()

        for copy in fetches(j, slot):
            copy.wait()

        @pl.when(j + 1 < n_steps)
        def _():
            for copy in fetches(j + 1, 1 - slot):
                copy.start()

    n = n_ref[...]
    g = g_ref[...]
    uv = dot_nn(n, w13[slot])
    da = dot_nt(g, w2c[slot])
    u = uv[:, :wide]
    v = uv[:, wide:]
    sig = jax.nn.sigmoid(u)
    up_act = u * sig
    act = (up_act * v).astype(BF16)
    du = (da * v * sig * (1.0 + u * (1.0 - sig))).astype(BF16)
    dv = (da * up_act).astype(BF16)
    du_0[...] = du[:, :sh]
    du_1[...] = du[:, sh:]
    dv_0[...] = dv[:, :sh]
    dv_1[...] = dv[:, sh:]

    @pl.when(jnp.logical_and(i == 0, j > 0))
    def _():
        finish(j - 1)

    ticks(j * n_tiles + i, n_tiles, MAIN[0], n_steps * n_tiles, *MAIN, 0, z_own, z_in, full, part, rest[24:])

    @pl.when(i == 0)
    def _():
        acc13[...] = jnp.zeros_like(acc13)
        acc2[...] = jnp.zeros_like(acc2)

    acc2[...] += dot_tn(act, g)
    acc13[...] += dot_tn(jnp.concatenate([du, dv], axis=1), n)

    @pl.when(i == n_tiles - 1)
    def _():
        local, remote = drains(j)
        for copy in remote + local:
            copy.start()

        @pl.when(j == n_steps - 1)
        def _():
            finish(j)


def sums(n_all, n_part, dim):
    block = (3 * UNIT, dim // 4)
    return ([jax.ShapeDtypeStruct((4, n_all, *block), F32)] if n_all else []) + ([jax.ShapeDtypeStruct((n_part, *block), F32)] if n_part else [])


def chunk_call(n, g, own, recv):
    tokens, dim = n.shape
    f_half = own[0].shape[1] // 2
    sh, tile = STEP, TILE
    n_steps, n_tiles = f_half // sh, tokens // tile
    tile_spec = pl.BlockSpec((tile, sh), lambda j, i: (i, j))
    row_spec = pl.BlockSpec((tile, dim), lambda j, i: (i, 0))
    big = jax.ShapeDtypeStruct((tokens, f_half), BF16)
    z = jax.ShapeDtypeStruct((3, f_half, dim), F32)
    return pl.pallas_call(
        functools.partial(chunk_kernel, sh, n_steps, n_tiles),
        grid=(n_steps, n_tiles),
        in_specs=[row_spec, row_spec] + [ANY] * 6,
        out_specs=[tile_spec] * 4 + [ANY] * 7,
        scratch_shapes=[
            pltpu.VMEM((2, dim, 4 * sh), BF16),
            pltpu.VMEM((2, 2 * sh, dim), BF16),
            pltpu.VMEM((4 * sh, dim), F32),
            pltpu.VMEM((2 * sh, dim), F32),
            pltpu.SemaphoreType.DMA((2, 10)),
            pltpu.SemaphoreType.DMA((5,)),
            pltpu.SemaphoreType.DMA((5,)),
            pltpu.SemaphoreType.DMA((n_steps, 5)),
            pltpu.SemaphoreType.DMA((2, 5)),
            pltpu.SemaphoreType.DMA((2, 5)),
        ] + rs_scratch(dim),
        out_shape=[big] * 4 + [z] * 2 + [jax.ShapeDtypeStruct(w.shape, BF16) for w in own] + sums(*MAIN, dim),
        input_output_aliases={5: 6, 6: 7, 7: 8},
        compiler_params=pltpu.CompilerParams(
            vmem_limit_bytes=VMEM_LIMIT, dimension_semantics=('arbitrary', 'arbitrary'), collective_id=0, has_side_effects=True),
        cost_estimate=pl.CostEstimate(flops=24 * tokens * dim * f_half, bytes_accessed=n_steps * 4 * tokens * dim + 24 * dim * f_half, transcendentals=tokens * 2 * f_half),
        name='chunks',
    )(n, g, *own, *recv)


def place_kernel(n_any, z, *rest):
    out1, out3, out2 = rest[n_any:]
    p = pl.program_id(1)
    _, n_units, _, eighth = z.shape
    rows = n_units * UNIT
    for r in range(4):
        x, y = r % 2, r // 2
        for half, index in ((0, 2 * x + y), (1, 2 * y + x)):
            @pl.when(p == half)
            def _():
                at = pl.ds(index * eighth, eighth)
                out1[at, :] = z[r, :, :UNIT, :].reshape(rows, eighth).T
                out3[at, :] = z[r, :, UNIT:2 * UNIT, :].reshape(rows, eighth).T
                out2[:, at] = z[r, :, 2 * UNIT:, :].reshape(rows, eighth)


def place_call(z, outs, after, half, f_half, first_unit, name):
    dim = 2 * half
    units = z.shape[1]
    group = 8 if units % 8 == 0 and first_unit % 8 == 0 else 4
    sb = group * UNIT
    first, f_blocks = first_unit // group, f_half // sb
    n_alias = len(outs)
    side = jax.ShapeDtypeStruct((half, 2 * f_half), F32)
    side_spec = pl.BlockSpec((half, sb), lambda j, p: (0, p * f_blocks + first + j))
    return pl.pallas_call(
        functools.partial(place_kernel, n_alias + len(after)),
        grid=(units // group, 2),
        in_specs=[pl.BlockSpec((4, group, 3 * UNIT, dim // 8), lambda j, p: (0, j, 0, p))] + [ANY] * (n_alias + len(after)),
        out_specs=[side_spec, side_spec, pl.BlockSpec((sb, half), lambda j, p: (first + j, p))],
        out_shape=[side, side, jax.ShapeDtypeStruct((f_half, dim), F32)],
        input_output_aliases={1 + a: a for a in range(n_alias)},
        compiler_params=pltpu.CompilerParams(vmem_limit_bytes=VMEM_LIMIT, dimension_semantics=('arbitrary', 'arbitrary')),
        cost_estimate=pl.CostEstimate(flops=3 * units * UNIT * dim, bytes_accessed=24 * units * UNIT * dim, transcendentals=0),
        name=name,
    )(z, *outs, *after)


def dn_kernel(n_tiles, n_steps, n_alias, n_all, n_part, first_unit, *refs):
    (du_0, du_1, dv_0, dv_1, w1o_0, w1o_1, w1r_0, w1r_1, w3o_0, w3o_1, w3r_0, w3r_1, h_ref, g_ref, z_own, z_in) = refs[:16]
    rest = refs[16 + n_alias:]
    out_ref = rest[0]
    full = rest[1] if n_all else None
    n_out = 1 + bool(n_all) + bool(n_part)
    part = rest[n_out - 1] if n_part else None
    acc_own, acc_oth = rest[n_out:n_out + 2]
    f = pl.program_id(1)
    half = acc_own.shape[1]
    step = pl.program_id(0) * n_steps + f
    enter(step)
    ticks(step, 0, n_all + n_part, n_tiles * n_steps, n_all, n_part, first_unit, z_own, z_in, full, part, rest[n_out + 2:])

    @pl.when(f == 0)
    def _():
        acc_own[...] = jnp.zeros_like(acc_own)
        acc_oth[...] = jnp.zeros_like(acc_oth)

    acc_own[...] += (dot_nt(du_0[...], w1o_0[...]) + dot_nt(du_1[...], w1o_1[...])
                     + dot_nt(dv_0[...], w3o_0[...]) + dot_nt(dv_1[...], w3o_1[...]))
    acc_oth[...] += (dot_nt(du_0[...], w1r_0[...]) + dot_nt(du_1[...], w1r_1[...])
                     + dot_nt(dv_0[...], w3r_0[...]) + dot_nt(dv_1[...], w3r_1[...]))

    @pl.when(f == n_steps - 1)
    def _():
        rows = 256
        first = lax.axis_index('fsdp') == 0
        for t in range(out_ref.shape[0] // rows):
            sl = pl.ds(t * rows, rows)
            h = h_ref[sl, :].astype(F32)
            inv_rms = lax.rsqrt(jnp.mean(h * h, axis=-1, keepdims=True) + NORM_EPS)
            y = h * inv_rms
            own, oth = acc_own[sl, :], acc_oth[sl, :]
            d = jnp.concatenate([jnp.where(first, own, oth), jnp.where(first, oth, own)], axis=1)
            mean = jnp.mean(d * y, axis=-1, keepdims=True)
            out_ref[sl, :] = (g_ref[sl, :].astype(F32) + inv_rms * (d - y * mean)).astype(BF16)


def dn_call(c, dus, w1o, w1r, w3o, w3r, h, g, z, bufs, tile_off, n_tiles, n_all, n_part, first_unit):
    tokens, dim = h.shape
    half = dim // 2
    tile, fb = 512, 512
    n_steps = dus[0].shape[1] // fb
    d_spec = pl.BlockSpec((tile, fb), lambda i, f: (tile_off + i, f))
    w_0 = pl.BlockSpec((half, fb), lambda i, f: (0, f))
    w_1 = pl.BlockSpec((half, fb), lambda i, f: (0, n_steps + f))
    row_spec = pl.BlockSpec((tile, dim), lambda i, f: (tile_off + i, 0))
    n_alias = len(bufs)
    out = sums(n_all, n_part, dim)
    return pl.pallas_call(
        functools.partial(dn_kernel, n_tiles, n_steps, n_alias, n_all, n_part, first_unit),
        grid=(n_tiles, n_steps),
        in_specs=[d_spec] * 4 + [w_0, w_1] * 4 + [row_spec, row_spec] + [ANY] * (2 + n_alias),
        out_specs=[row_spec] + [ANY] * len(out),
        scratch_shapes=[pltpu.VMEM((tile, half), F32), pltpu.VMEM((tile, half), F32)] + rs_scratch(dim),
        out_shape=[jax.ShapeDtypeStruct((tokens, dim), BF16)] + out,
        input_output_aliases={16 + a: a for a in range(n_alias)},
        compiler_params=pltpu.CompilerParams(vmem_limit_bytes=VMEM_LIMIT, dimension_semantics=('arbitrary', 'arbitrary'), collective_id=c, has_side_effects=True),
        cost_estimate=pl.CostEstimate(flops=8 * n_tiles * tile * dim * n_steps * fb, bytes_accessed=8 * n_tiles * tile * n_steps * fb + 8 * n_tiles * dim * n_steps * fb, transcendentals=tokens),
        name=f'dn{tile_off}',
    )(*dus, w1o, w1o, w1r, w1r, w3o, w3o, w3r, w3r, h, g, *z, *bufs)


def copy_kernel(src, dst):
    dst[...] = src[...]


def copy_call(x):
    spec = pl.BlockSpec((512, x.shape[1]), lambda i: (i, 0))
    return pl.pallas_call(
        copy_kernel, grid=(x.shape[0] // 512,), in_specs=[spec], out_specs=spec, out_shape=jax.ShapeDtypeStruct(x.shape, x.dtype),
        cost_estimate=pl.CostEstimate(flops=x.size, bytes_accessed=4 * x.size, transcendentals=0), name='out')(x)


def solution(mesh):
    tok_spec = P(('replica', 'fsdp'), None)
    act_spec = P(None, ('replica', 'fsdp'), None)
    weight_spec = P(None, 'fsdp', None)

    def local_step(block_in, grad_out, w_up, w_lin, w_down):
        h, g = block_in[0], grad_out
        own = (w_up[0], w_lin[0], w_down[0])
        half, ff = own[0].shape
        fh = ff // 2

        def gather(part):
            return lax.all_gather(part, 'replica', axis=0, tiled=True).reshape(4, *part.shape)

        n, *recv = norm_call(h, own)
        *dus, z_own, z_in, w1r, w3r, _, full, part = chunk_call(n, g, own, recv)
        placed = [(0, full)]
        late = [(MAIN[0], gather(part))]
        first, tile_off = sum(MAIN), 0
        dh = ()
        for c, (tiles, n_all, n_part) in enumerate(TAILS):
            dh, *res = dn_call(1 + c, dus, own[0], w1r, own[1], w3r, h, g, (z_own, z_in), dh, tile_off, tiles, n_all, n_part, first)
            dh = (dh,)
            if n_all:
                placed.append((first, res[0]))
            if n_part:
                late.append((first + n_all, gather(res[-1])))
            tile_off += tiles
            first += n_all + n_part
        dh = copy_call(dh[0])
        outs = ()
        jobs = placed + late
        for i, (unit, sums_of) in enumerate(jobs):
            after = (dh,) if i == len(jobs) - 1 else ()
            outs = tuple(place_call(sums_of, outs, after, half, fh, unit, f'place{unit}'))
        return outs[0][None], outs[1][None], outs[2][None], dh

    return jax.shard_map(local_step, mesh=mesh, in_specs=(act_spec, tok_spec, weight_spec, weight_spec, weight_spec), out_specs=(weight_spec, weight_spec, weight_spec, tok_spec), check_vma=False)
```

```python
import functools

import jax
import jax.numpy as jnp
from jax import lax
from jax.experimental import pallas as pl
from jax.experimental.pallas import tpu as pltpu
from jax.sharding import PartitionSpec as P

NORM_EPS = 1e-5
BF16 = jnp.bfloat16
F32 = jnp.float32
VMEM_LIMIT = 62 * 1024 * 1024
UNIT = 32
SLOTS = 4
F_SLOTS = 8
G_SLOTS = 16
STEP = 256
MAIN = 88
TAIL = (24, 16)
FINISH = 3
FAST = 8
EARLY = (512, 2048)
TILE = 512
ANY = pl.BlockSpec(memory_space=pl.ANY)
MESH = pl.DeviceIdType.MESH


def SMALL():
    global STEP, MAIN, TAIL, EARLY, FINISH, FAST
    STEP, MAIN, TAIL, EARLY, FINISH, FAST = 128, 16, (8, 8), (256, 512), 1, 2


def dot_nn(a, b):
    return lax.dot_general(a, b, (((1,), (0,)), ((), ())), preferred_element_type=F32)


def dot_nt(a, b):
    return lax.dot_general(a, b, (((1,), (1,)), ((), ())), preferred_element_type=F32)


def dot_tn(a, b):
    return lax.dot_general(a, b, (((0,), (0,)), ((), ())), preferred_element_type=F32)


def exchange(w1o, w3o, w2o, into, lo, hi, send_sem, recv_sem):
    r, k, _, _ = position()
    f_half = w1o.shape[1] // 2
    pairs = [(src.at[:, pl.ds(p * f_half + lo, hi - lo)], dst.at[:, pl.ds(p * f_half + lo, hi - lo)])
             for src, dst in ((w1o, into[0]), (w3o, into[1])) for p in range(2)]
    pairs.append((w2o.at[pl.ds(lo, hi - lo), :], into[2].at[pl.ds(lo, hi - lo), :]))
    return [pltpu.make_async_remote_copy(
        src_ref=src, dst_ref=dst, send_sem=send_sem.at[num], recv_sem=recv_sem.at[num],
        device_id=(r, 1 - k), device_id_type=MESH) for num, (src, dst) in enumerate(pairs)]


def norm_kernel(n_tiles, h_ref, w1o, w3o, w2o, n_ref, w1r, w3r, w2r, send_sem, recv_sem):
    i = pl.program_id(0)
    r, k, _, _ = position()
    args = (w1o, w3o, w2o, (w1r, w3r, w2r), 0, EARLY[0], send_sem, recv_sem)

    @pl.when(i == 0)
    def _():
        barrier = pltpu.get_barrier_semaphore()
        pl.semaphore_signal(barrier, inc=1, device_id=(r, 1 - k), device_id_type=MESH)
        pl.semaphore_wait(barrier, 1)
        for copy in exchange(*args):
            copy.start()

    half = h_ref.shape[1] // 2
    h = h_ref[...].astype(F32)
    inv_rms = lax.rsqrt(jnp.mean(h * h, axis=-1, keepdims=True) + NORM_EPS)
    y = (h * inv_rms).astype(BF16)
    first = k == 0
    n_ref[:, :half] = jnp.where(first, y[:, :half], y[:, half:])
    n_ref[:, half:] = jnp.where(first, y[:, half:], y[:, :half])

    @pl.when(i == n_tiles - 1)
    def _():
        for copy in exchange(*args):
            copy.wait()


def norm_call(h, own):
    tokens, dim = h.shape
    tile = 512
    spec = pl.BlockSpec((tile, dim), lambda i: (i, 0))
    return pl.pallas_call(
        functools.partial(norm_kernel, tokens // tile),
        grid=(tokens // tile,),
        in_specs=[spec] + [ANY] * 3,
        out_specs=[spec] + [ANY] * 3,
        scratch_shapes=[pltpu.SemaphoreType.DMA((5,)), pltpu.SemaphoreType.DMA((5,))],
        out_shape=[jax.ShapeDtypeStruct((tokens, dim), BF16)] + [jax.ShapeDtypeStruct(w.shape, BF16) for w in own],
        compiler_params=pltpu.CompilerParams(vmem_limit_bytes=VMEM_LIMIT, collective_id=8, has_side_effects=True),
        cost_estimate=pl.CostEstimate(flops=6 * tokens * dim, bytes_accessed=4 * tokens * dim, transcendentals=tokens),
        name='norm',
    )(h, *own)


def rs_scratch(dim):
    rows = 3 * UNIT
    return [
        pltpu.VMEM((SLOTS, rows, dim), F32),
        pltpu.VMEM((SLOTS, rows, dim), F32),
        pltpu.VMEM((SLOTS, rows, dim // 2), F32),
        pltpu.VMEM((SLOTS, rows, dim // 2), F32),
        pltpu.VMEM((SLOTS, rows, dim // 4), F32),
        pltpu.VMEM((F_SLOTS, rows, dim // 4), F32),
        pltpu.SemaphoreType.DMA((SLOTS, 6)),
        pltpu.SemaphoreType.DMA((SLOTS, 4)),
        pltpu.SemaphoreType.DMA((SLOTS, 4)),
        pltpu.SemaphoreType.DMA((F_SLOTS, 2)),
        pltpu.SemaphoreType.DMA((G_SLOTS, 6)),
        pltpu.SemaphoreType.DMA((G_SLOTS, 6)),
        pltpu.SemaphoreType.REGULAR((4,)),
    ]


def position():
    r = lax.axis_index('replica')
    k = lax.axis_index('fsdp')
    x, y = lax.rem(r, 2), lax.div(r, 2)
    return r, k, x, y


def enter(step):
    r, k, x, y = position()

    @pl.when(step == 0)
    def _():
        barrier = pltpu.get_barrier_semaphore()
        for peer in ((r, 1 - k), (r + 1 - 2 * x, k), (r + 2 - 4 * y, k)):
            pl.semaphore_signal(barrier, inc=1, device_id=peer, device_id_type=MESH)
        pl.semaphore_wait(barrier, 3)


def ticks(step, begin, fast, n_lead, n_grid, n_all, n_part, first, z_own, z_in, full, part, scratch):
    own_buf, in_buf, r1, y2, r2, f_buf, load_sem, send_sem, recv_sem, out_sem, g_send, g_recv, credit = scratch
    r, k, x, y = position()
    at_x, at_y = (r + 1 - 2 * x, k), (r + 2 - 4 * y, k)
    dim = own_buf.shape[2]
    quarter, eighth = dim // 4, dim // 8
    n_units = n_all + n_part
    n_ticks = max(n_all + 11, n_units + 7) if n_all else n_units + 7

    def loads(u):
        slot = lax.rem(u, SLOTS)
        row = pl.multiple_of((first + u) * UNIT, UNIT)
        copies = []
        for part in range(3):
            dst = pl.ds(part * UNIT, UNIT)
            copies.append(pltpu.make_async_copy(z_own.at[part, pl.ds(row, UNIT), :], own_buf.at[slot, dst, :], load_sem.at[slot, part]))
            copies.append(pltpu.make_async_copy(z_in.at[part, pl.ds(row, UNIT), :], in_buf.at[slot, dst, :], load_sem.at[slot, 3 + part]))
        return copies

    def lanes(base, index, width):
        return pl.ds(pl.multiple_of(base + index * width, 128), width)

    def first_hop(u):
        slot = lax.rem(u, SLOTS)
        out = []
        for i, (base, index, peer, col) in enumerate(((0, 1 - x, at_x, 0), (dim // 2, 1 - y, at_y, quarter))):
            out.append(pltpu.make_async_remote_copy(
                src_ref=own_buf.at[slot, :, lanes(base, index, quarter)], dst_ref=r1.at[slot, :, pl.ds(col, quarter)],
                send_sem=send_sem.at[slot, i], recv_sem=recv_sem.at[slot, i], device_id=peer, device_id_type=MESH))
        return out

    def second_hop(u):
        slot = lax.rem(u, SLOTS)
        out = []
        for i, (base, index, peer, col) in enumerate(((0, 1 - y, at_y, 0), (quarter, 1 - x, at_x, eighth))):
            out.append(pltpu.make_async_remote_copy(
                src_ref=y2.at[slot, :, lanes(base, index, eighth)], dst_ref=r2.at[slot, :, pl.ds(col, eighth)],
                send_sem=send_sem.at[slot, 2 + i], recv_sem=recv_sem.at[slot, 2 + i], device_id=peer, device_id_type=MESH))
        return out

    def store_all(u):
        slot = lax.rem(u, F_SLOTS)
        return pltpu.make_async_copy(f_buf.at[slot], full.at[r, u], out_sem.at[slot, 0])

    def store_part(u):
        slot = lax.rem(u, F_SLOTS)
        return [pltpu.make_async_copy(f_buf.at[slot, :, pl.ds(i * eighth, eighth)], part[i].at[u - n_all], out_sem.at[slot, i]) for i in range(2)]

    def spread(u, num, src, origin, col, peer):
        slot = lax.rem(u, G_SLOTS)
        return pltpu.make_async_remote_copy(
            src_ref=src, dst_ref=full.at[origin, u, :, pl.ds(col, eighth)], send_sem=g_send.at[slot, num],
            recv_sem=g_recv.at[slot, num], device_id=peer, device_id_type=MESH)

    def third_hop(u):
        slot = lax.rem(u, F_SLOTS)
        return [spread(u, i, f_buf.at[slot, :, pl.ds(col, eighth)], r, col, peer)
                for i, (col, peer) in enumerate(((0, at_y), (eighth, at_x)))]

    def fourth_hop(u):
        slot = lax.rem(u, F_SLOTS)
        return [spread(u, 2 + i, f_buf.at[slot, :, pl.ds(col, eighth)], r, col, peer)
                for i, (col, peer) in enumerate(((0, at_x), (eighth, at_y)))]

    def forward(u):
        return [spread(u, 4 + i, full.at[origin, u, :, pl.ds(col, eighth)], origin, col, peer)
                for i, (origin, col, peer) in enumerate(((at_y[0], 0, at_x), (at_x[0], eighth, at_y)))]

    def stage(tick, lag, fn, lo=0, hi=n_units):
        if lo < hi:
            u = tick - lag

            @pl.when(jnp.logical_and(u >= lo, u < hi))
            def _():
                fn(u, lax.rem(u, SLOTS))

    def do_load(u, slot):
        for copy in loads(u):
            copy.start()

    def do_first(u, slot):
        for copy in loads(u):
            copy.wait()
        own_buf[slot] = own_buf[slot] + in_buf[slot]

        @pl.when(u >= SLOTS)
        def _():
            pl.semaphore_wait(credit.at[0], 1)
            pl.semaphore_wait(credit.at[1], 1)

        for copy in first_hop(u):
            copy.start()

    def do_second(u, slot):
        for copy in first_hop(u):
            copy.wait()
        y2[slot, :, :quarter] = own_buf[slot, :, lanes(0, x, quarter)] + r1[slot, :, :quarter]
        y2[slot, :, quarter:] = own_buf[slot, :, lanes(dim // 2, y, quarter)] + r1[slot, :, quarter:]

        @pl.when(u < n_units - SLOTS)
        def _():
            pl.semaphore_signal(credit.at[0], inc=1, device_id=at_x, device_id_type=MESH)
            pl.semaphore_signal(credit.at[1], inc=1, device_id=at_y, device_id_type=MESH)

        @pl.when(u >= SLOTS)
        def _():
            pl.semaphore_wait(credit.at[2], 1)
            pl.semaphore_wait(credit.at[3], 1)

        for copy in second_hop(u):
            copy.start()

    def do_third(u, slot):
        for copy in second_hop(u):
            copy.wait()
        f_slot = lax.rem(u, F_SLOTS)
        f_buf[f_slot, :, :eighth] = y2[slot, :, lanes(0, y, eighth)] + r2[slot, :, :eighth]
        f_buf[f_slot, :, eighth:] = y2[slot, :, lanes(quarter, x, eighth)] + r2[slot, :, eighth:]

        @pl.when(u < n_units - SLOTS)
        def _():
            pl.semaphore_signal(credit.at[2], inc=1, device_id=at_y, device_id_type=MESH)
            pl.semaphore_signal(credit.at[3], inc=1, device_id=at_x, device_id_type=MESH)

        if n_all:
            @pl.when(u < n_all)
            def _():
                store_all(u).start()
                for copy in third_hop(u) + fourth_hop(u):
                    copy.start()

        if n_part:
            @pl.when(u >= n_all)
            def _():
                for copy in store_part(u):
                    copy.start()

    def do_forward(u, slot):
        for copy in third_hop(u):
            copy.wait()
        for copy in forward(u):
            copy.start()

    def end_all(u, slot):
        store_all(u).wait()
        for copy in fourth_hop(u) + forward(u):
            copy.wait()

    def end_part(u, slot):
        for copy in store_part(u):
            copy.wait()

    def tick(t, carry):
        stage(t, 10, end_all, 0, n_all)
        stage(t, 7, do_forward, 0, n_all)
        stage(t, 6, end_part, n_all, n_units)
        stage(t, 5, do_third)
        stage(t, 3, do_second)
        stage(t, 1, do_first)
        stage(t, 0, do_load)
        return carry

    spread_steps = n_grid - FINISH - begin - fast
    lead = n_lead + 1
    late = step // (n_grid - FINISH)
    filling = 1 // (1 + step // (begin + fast)) if fast else 0

    def bound(at):
        ahead = at - begin
        here = filling * ahead + (1 - filling) * (fast + ((ahead - fast) * (lead - fast)) // spread_steps)
        there = lead + ((at - (n_grid - FINISH)) * (n_ticks - lead)) // FINISH
        return (1 - late) * here + late * there

    @pl.when(step >= begin)
    def _():
        lax.fori_loop(bound(step), bound(step + 1), tick, 0)


def chunk_kernel(sh, n_steps, n_tiles, n_ref, g_ref, w1o, w3o, w2o, *rest):
    du_0, du_1, dv_0, dv_1, z_own, z_in, w1r, w3r, w2r, full = rest[3:13]
    w13, w2c, acc13, acc2, w_sem, out_sem, d_send, d_recv, p_send, p_recv = rest[13:23]
    half = w1o.shape[0]
    f_half = w1o.shape[1] // 2
    wide = 2 * sh
    j = pl.program_id(0)
    i = pl.program_id(1)
    slot = lax.rem(j, 2)
    r, k, _, _ = position()
    own_row = pl.multiple_of(k * sh, 128)
    oth_row = pl.multiple_of((1 - k) * sh, 128)
    enter(j * n_tiles + i)
    def fetches(step, buf):
        copies = []

        def add(src, dst):
            copies.append(pltpu.make_async_copy(src, dst, w_sem.at[buf, len(copies)]))

        at = pl.multiple_of(step * sh, 128)
        for own_src, oth_src, col in ((w1o, w1r, 0), (w3o, w3r, wide)):
            for src, row in ((own_src, 0), (oth_src, half)):
                for p in range(2):
                    add(src.at[:, pl.ds(p * f_half + at, sh)], w13.at[buf, pl.ds(row, half), pl.ds(col + p * sh, sh)])
        for src, row in ((w2o, own_row), (w2r, oth_row)):
            add(src.at[pl.ds(at, sh), :], w2c.at[buf, pl.ds(row, sh), :])
        return copies

    def drains(step):
        row = pl.multiple_of(step * sh, 128)
        local, remote = [], []

        def add(keep, send, part, lanes):
            num = len(local)
            local.append(pltpu.make_async_copy(keep, z_own.at[part, pl.ds(row, sh), lanes], out_sem.at[num]))
            remote.append(pltpu.make_async_remote_copy(
                src_ref=send, dst_ref=z_in.at[part, pl.ds(row, sh), lanes], send_sem=d_send.at[num], recv_sem=d_recv.at[step, num],
                device_id=(r, 1 - k), device_id_type=MESH))

        for part in range(2):
            for p in range(2):
                src = pl.ds(part * wide + p * sh, sh)
                add(acc13.at[src, pl.ds(0, half)], acc13.at[src, pl.ds(half, half)], part, pl.ds(p * half, half))
        add(acc2.at[pl.ds(own_row, sh), :], acc2.at[pl.ds(oth_row, sh), :], 2, pl.ds(0, 2 * half))
        return local, remote

    def finish(step):
        local, remote = drains(step)
        for copy in local:
            copy.wait()
        for copy in remote:
            copy.wait()

    for num, (lo, hi, at) in enumerate(((*EARLY, (0, 0)), (EARLY[1], f_half, (1, n_tiles // 2)))):
        args = (w1o, w3o, w2o, (w1r, w3r, w2r), lo, hi, p_send.at[num], p_recv.at[num])

        @pl.when(jnp.logical_and(j == at[0], i == at[1]))
        def _():
            for copy in exchange(*args):
                copy.start()

        @pl.when(jnp.logical_and(j == lo // sh - 1, i == 0))
        def _():
            for copy in exchange(*args):
                copy.wait()

    @pl.when(i == 0)
    def _():
        @pl.when(j == 0)
        def _():
            for copy in fetches(0, 0):
                copy.start()

        for copy in fetches(j, slot):
            copy.wait()

        @pl.when(j + 1 < n_steps)
        def _():
            for copy in fetches(j + 1, 1 - slot):
                copy.start()

    n = n_ref[...]
    g = g_ref[...]
    uv = dot_nn(n, w13[slot])
    da = dot_nt(g, w2c[slot])
    u = uv[:, :wide]
    v = uv[:, wide:]
    sig = jax.nn.sigmoid(u)
    up_act = u * sig
    act = (up_act * v).astype(BF16)
    du = (da * v * sig * (1.0 + u * (1.0 - sig))).astype(BF16)
    dv = (da * up_act).astype(BF16)
    du_0[...] = du[:, :sh]
    du_1[...] = du[:, sh:]
    dv_0[...] = dv[:, :sh]
    dv_1[...] = dv[:, sh:]

    @pl.when(jnp.logical_and(i == 0, j > 0))
    def _():
        finish(j - 1)

    ticks(j * n_tiles + i, n_tiles, FAST, MAIN, n_steps * n_tiles, MAIN, 0, 0, z_own, z_in, full, None, rest[23:])

    @pl.when(i == 0)
    def _():
        acc13[...] = jnp.zeros_like(acc13)
        acc2[...] = jnp.zeros_like(acc2)

    acc2[...] += dot_tn(act, g)
    acc13[...] += dot_tn(jnp.concatenate([du, dv], axis=1), n)

    @pl.when(i == n_tiles - 1)
    def _():
        local, remote = drains(j)
        for copy in remote + local:
            copy.start()

        @pl.when(j == n_steps - 1)
        def _():
            finish(j)


def sums(n_all, n_part, dim):
    rows = 3 * UNIT
    return [jax.ShapeDtypeStruct((4, n_all, rows, dim // 4), F32)] + [jax.ShapeDtypeStruct((n_part, rows, dim // 8), F32)] * (2 * bool(n_part))


def chunk_call(n, g, own, recv):
    tokens, dim = n.shape
    f_half = own[0].shape[1] // 2
    sh, tile = STEP, TILE
    n_steps, n_tiles = f_half // sh, tokens // tile
    tile_spec = pl.BlockSpec((tile, sh), lambda j, i: (i, j))
    row_spec = pl.BlockSpec((tile, dim), lambda j, i: (i, 0))
    big = jax.ShapeDtypeStruct((tokens, f_half), BF16)
    z = jax.ShapeDtypeStruct((3, f_half, dim), F32)
    return pl.pallas_call(
        functools.partial(chunk_kernel, sh, n_steps, n_tiles),
        grid=(n_steps, n_tiles),
        in_specs=[row_spec, row_spec] + [ANY] * 6,
        out_specs=[tile_spec] * 4 + [ANY] * 6,
        scratch_shapes=[
            pltpu.VMEM((2, dim, 4 * sh), BF16),
            pltpu.VMEM((2, 2 * sh, dim), BF16),
            pltpu.VMEM((4 * sh, dim), F32),
            pltpu.VMEM((2 * sh, dim), F32),
            pltpu.SemaphoreType.DMA((2, 10)),
            pltpu.SemaphoreType.DMA((5,)),
            pltpu.SemaphoreType.DMA((5,)),
            pltpu.SemaphoreType.DMA((n_steps, 5)),
            pltpu.SemaphoreType.DMA((2, 5)),
            pltpu.SemaphoreType.DMA((2, 5)),
        ] + rs_scratch(dim),
        out_shape=[big] * 4 + [z] * 2 + [jax.ShapeDtypeStruct(w.shape, BF16) for w in own] + sums(MAIN, 0, dim),
        input_output_aliases={5: 6, 6: 7, 7: 8},
        compiler_params=pltpu.CompilerParams(
            vmem_limit_bytes=VMEM_LIMIT, dimension_semantics=('arbitrary', 'arbitrary'), collective_id=0, has_side_effects=True),
        cost_estimate=pl.CostEstimate(flops=24 * tokens * dim * f_half, bytes_accessed=n_steps * 4 * tokens * dim + 24 * dim * f_half, transcendentals=tokens * 2 * f_half),
        name='chunks',
    )(n, g, *own, *recv)


def place_kernel(n_any, z, *rest):
    out1, out3, out2 = rest[n_any:]
    p = pl.program_id(1)
    _, n_units, _, eighth = z.shape
    rows = n_units * UNIT
    for r in range(4):
        x, y = r % 2, r // 2
        for half, index in ((0, 2 * x + y), (1, 2 * y + x)):
            @pl.when(p == half)
            def _():
                at = pl.ds(index * eighth, eighth)
                out1[at, :] = z[r, :, :UNIT, :].reshape(rows, eighth).T
                out3[at, :] = z[r, :, UNIT:2 * UNIT, :].reshape(rows, eighth).T
                out2[:, at] = z[r, :, 2 * UNIT:, :].reshape(rows, eighth)


def place_pieces_kernel(n_any, *refs):
    pieces, (out1, out3, out2) = refs[:8], refs[8 + n_any:]
    _, _, x, y = position()
    p = pl.program_id(1)
    n_units, _, eighth = pieces[0].shape
    rows = n_units * UNIT
    for half, (a, b) in enumerate(((x, y), (y, x))):
        @pl.when(p == half)
        def _():
            for num, index in enumerate((2 * a + b, 2 * a + 1 - b, 2 * (1 - a) + b, 2 * (1 - a) + 1 - b)):
                z = pieces[4 * half + num]
                at = pl.ds(pl.multiple_of(index * eighth, eighth), eighth)
                out1[at, :] = z[:, :UNIT, :].reshape(rows, eighth).T
                out3[at, :] = z[:, UNIT:2 * UNIT, :].reshape(rows, eighth).T
                out2[:, at] = z[:, 2 * UNIT:, :].reshape(rows, eighth)


def place_call(z, outs, after, half, f_half, first_unit, name):
    dim = 2 * half
    pieces = isinstance(z, tuple)
    units = z[0].shape[0] if pieces else z.shape[1]
    group = 8 if units % 8 == 0 and first_unit % 8 == 0 else 4
    sb = group * UNIT
    first, f_blocks = first_unit // group, f_half // sb
    n_alias = len(outs)
    side = jax.ShapeDtypeStruct((half, 2 * f_half), F32)
    side_spec = pl.BlockSpec((half, sb), lambda j, p: (0, p * f_blocks + first + j))
    if pieces:
        kernel, in_specs = place_pieces_kernel, [pl.BlockSpec((group, 3 * UNIT, dim // 8), lambda j, p: (j, 0, 0))] * 8
    else:
        kernel, in_specs = place_kernel, [pl.BlockSpec((4, group, 3 * UNIT, dim // 8), lambda j, p: (0, j, 0, p))]
        z = (z,)
    return pl.pallas_call(
        functools.partial(kernel, n_alias + len(after)),
        grid=(units // group, 2),
        in_specs=in_specs + [ANY] * (n_alias + len(after)),
        out_specs=[side_spec, side_spec, pl.BlockSpec((sb, half), lambda j, p: (first + j, p))],
        out_shape=[side, side, jax.ShapeDtypeStruct((f_half, dim), F32)],
        input_output_aliases={len(z) + a: a for a in range(n_alias)},
        compiler_params=pltpu.CompilerParams(vmem_limit_bytes=VMEM_LIMIT, dimension_semantics=('arbitrary', 'arbitrary')),
        cost_estimate=pl.CostEstimate(flops=60 * units * UNIT * dim, bytes_accessed=24 * units * UNIT * dim, transcendentals=0),
        name=name,
    )(*z, *outs, *after)


def dn_kernel(n_tiles, n_steps, n_alias, n_all, n_part, first_unit, *refs):
    (du_0, du_1, dv_0, dv_1, w1o_0, w1o_1, w1r_0, w1r_1, w3o_0, w3o_1, w3r_0, w3r_1, h_ref, g_ref, z_own, z_in) = refs[:16]
    rest = refs[16 + n_alias:]
    out_ref = rest[0]
    full, part = rest[1], rest[2:4]
    n_out = 4
    acc_own, acc_oth = rest[n_out:n_out + 2]
    f = pl.program_id(1)
    half = acc_own.shape[1]
    step = pl.program_id(0) * n_steps + f
    enter(step)
    ticks(step, 0, 0, n_all, n_tiles * n_steps, n_all, n_part, first_unit, z_own, z_in, full, part, rest[n_out + 2:])

    @pl.when(f == 0)
    def _():
        acc_own[...] = jnp.zeros_like(acc_own)
        acc_oth[...] = jnp.zeros_like(acc_oth)

    acc_own[...] += (dot_nt(du_0[...], w1o_0[...]) + dot_nt(du_1[...], w1o_1[...])
                     + dot_nt(dv_0[...], w3o_0[...]) + dot_nt(dv_1[...], w3o_1[...]))
    acc_oth[...] += (dot_nt(du_0[...], w1r_0[...]) + dot_nt(du_1[...], w1r_1[...])
                     + dot_nt(dv_0[...], w3r_0[...]) + dot_nt(dv_1[...], w3r_1[...]))

    @pl.when(f == n_steps - 1)
    def _():
        rows = 256
        first = lax.axis_index('fsdp') == 0
        for t in range(out_ref.shape[0] // rows):
            sl = pl.ds(t * rows, rows)
            h = h_ref[sl, :].astype(F32)
            inv_rms = lax.rsqrt(jnp.mean(h * h, axis=-1, keepdims=True) + NORM_EPS)
            y = h * inv_rms
            own, oth = acc_own[sl, :], acc_oth[sl, :]
            d = jnp.concatenate([jnp.where(first, own, oth), jnp.where(first, oth, own)], axis=1)
            mean = jnp.mean(d * y, axis=-1, keepdims=True)
            out_ref[sl, :] = (g_ref[sl, :].astype(F32) + inv_rms * (d - y * mean)).astype(BF16)


def dn_call(c, dus, w1o, w1r, w3o, w3r, h, g, z, bufs, tile_off, n_tiles, n_all, n_part, first_unit):
    tokens, dim = h.shape
    half = dim // 2
    tile, fb = 512, 512
    n_steps = dus[0].shape[1] // fb
    d_spec = pl.BlockSpec((tile, fb), lambda i, f: (tile_off + i, f))
    w_0 = pl.BlockSpec((half, fb), lambda i, f: (0, f))
    w_1 = pl.BlockSpec((half, fb), lambda i, f: (0, n_steps + f))
    row_spec = pl.BlockSpec((tile, dim), lambda i, f: (tile_off + i, 0))
    n_alias = len(bufs)
    out = sums(n_all, n_part, dim)
    return pl.pallas_call(
        functools.partial(dn_kernel, n_tiles, n_steps, n_alias, n_all, n_part, first_unit),
        grid=(n_tiles, n_steps),
        in_specs=[d_spec] * 4 + [w_0, w_1] * 4 + [row_spec, row_spec] + [ANY] * (2 + n_alias),
        out_specs=[row_spec] + [ANY] * len(out),
        scratch_shapes=[pltpu.VMEM((tile, half), F32), pltpu.VMEM((tile, half), F32)] + rs_scratch(dim),
        out_shape=[jax.ShapeDtypeStruct((tokens, dim), BF16)] + out,
        input_output_aliases={16 + a: a for a in range(n_alias)},
        compiler_params=pltpu.CompilerParams(vmem_limit_bytes=VMEM_LIMIT, dimension_semantics=('arbitrary', 'arbitrary'), collective_id=c, has_side_effects=True),
        cost_estimate=pl.CostEstimate(flops=8 * n_tiles * tile * dim * n_steps * fb, bytes_accessed=8 * n_tiles * tile * n_steps * fb + 8 * n_tiles * dim * n_steps * fb, transcendentals=tokens),
        name=f'dn{tile_off}',
    )(*dus, w1o, w1o, w1r, w1r, w3o, w3o, w3r, w3r, h, g, *z, *bufs)


def copy_kernel(src, dst):
    dst[...] = src[...]


def copy_call(x):
    spec = pl.BlockSpec((512, x.shape[1]), lambda i: (i, 0))
    return pl.pallas_call(
        copy_kernel, grid=(x.shape[0] // 512,), in_specs=[spec], out_specs=spec, out_shape=jax.ShapeDtypeStruct(x.shape, x.dtype),
        cost_estimate=pl.CostEstimate(flops=x.size, bytes_accessed=4 * x.size, transcendentals=0), name='out')(x)


def solution(mesh):
    tok_spec = P(('replica', 'fsdp'), None)
    act_spec = P(None, ('replica', 'fsdp'), None)
    weight_spec = P(None, 'fsdp', None)

    def local_step(block_in, grad_out, w_up, w_lin, w_down):
        h, g = block_in[0], grad_out
        own = (w_up[0], w_lin[0], w_down[0])
        half, ff = own[0].shape
        fh = ff // 2

        def over(bit, v):
            return lax.ppermute(v, 'replica', [(r, r ^ bit) for r in range(4)])

        n, *recv = norm_call(h, own)
        *dus, z_own, z_in, w1r, w3r, _, full = chunk_call(n, g, own, recv)
        dh, full_2, a, b = dn_call(1, dus, own[0], w1r, own[1], w3r, h, g, (z_own, z_in), (), 0, h.shape[0] // 512, *TAIL, MAIN)
        a_y, b_x = over(2, a), over(1, b)
        a_x, b_y = over(1, a), over(2, b)
        dh = copy_call(dh)
        outs = place_call(full_2, (), (dh,), half, fh, MAIN, 'place1')
        a_y, b_x, *outs = lax.optimization_barrier((a_y, b_x, *outs))
        a_d, b_d = over(1, a_y), over(2, b_x)
        outs = place_call(full, tuple(outs), (), half, fh, 0, 'place0')
        outs = place_call((a, a_y, a_x, a_d, b, b_x, b_y, b_d), tuple(outs), (), half, fh, MAIN + TAIL[0], 'place2')
        return outs[0][None], outs[1][None], outs[2][None], dh

    return jax.shard_map(local_step, mesh=mesh, in_specs=(act_spec, tok_spec, weight_spec, weight_spec, weight_spec), out_specs=(weight_spec, weight_spec, weight_spec, tok_spec), check_vma=False)
```
